128 devices in a mesh: seq: 32 (over y, z, core), dp: 4 (over x).
Axes of the slice: x: 4, y: 4, z: 4, core: 2. Of those that a mesh axis runs over, the one named last changes fastest.
Arguments:
- query_input: bfloat16 [4, 16384, 2048], P('dp', 'seq'), may hold values from -6 to 6
- key_input: bfloat16 [4, 16384, 2048], P('dp', 'seq'), may hold values from -6 to 6
- value_input: bfloat16 [4, 16384, 2048], P('dp', 'seq'), may hold values from -6 to 6
- grad_output: bfloat16 [4, 16384, 2048], P('dp', 'seq'), may hold values from -6 to 6
- out_weight: bfloat16 [2048, 2048], P(('seq', 'dp')), may hold values from -0.125 to 0.125
- norm_gain: float32 [2048], replicated, may hold values from 0.1 to 1.9
Outputs:
- result: bfloat16 [4, 16384, 2048], P('dp', 'seq')
- grad_query: bfloat16 [4, 16384, 2048], P('dp', 'seq')
- grad_key: bfloat16 [4, 16384, 2048], P('dp', 'seq')
- grad_value: bfloat16 [4, 16384, 2048], P('dp', 'seq')
- grad_weight: float32 [2048, 2048], P(('seq', 'dp'))
The draws below stay inside these ranges and needn't reach their ends.
All inputs are finite; a program needn't handle non-finite values.
Results may differ from the reference program's by a relative error of at most 0.015.
Values may be sent and summed in bfloat16 or wider, within the bound.
No kernel may reach another device: no remote copies, remote signals or barrier semaphores. Data moves between devices by JAX's collectives and lax.ppermute only.
A program may use at most 192 MiB of HBM per device.

```python
import jax
import jax.numpy as jnp
from jax import lax

HEADS = 16
HEAD_DIM = 128
OUT_COLS = 2048
BLOCK = 512
FEATURES = 2048
LENGTH = 16384
BATCH = 4


def level_of(stream_key, dims, cuts, low, top_value):
    def one(axis_at, blocks):
        draws = jax.random.uniform(jax.random.fold_in(jax.random.fold_in(stream_key, 6), axis_at), (blocks,), jnp.float32, low / len(cuts), top_value / len(cuts))
        return jnp.repeat(jnp.exp(draws), dims[axis_at] // blocks).reshape((-1,) + (1,) * (len(dims) - axis_at - 1))

    level = one(*cuts[0])
    for cut in cuts[1:]:
        level = level * one(*cut)
    return level


def bell_draw(key, shape, spread, reach, shards=(), dtype=jnp.bfloat16):
    values = spread * jax.random.normal(key, shape, jnp.float32)
    if shards:
        values = values * level_of(key, shape, shards, -0.22, 0.18)
    return jnp.clip(values, -reach, reach).astype(dtype)


def setup_inputs(seed: int = 0) -> dict:
    key_of = jax.random.split(jax.random.key(seed), 7)
    return {
        "query_input": bell_draw(key_of[0], (BATCH, LENGTH, FEATURES), 1.0, 6.0, ((0, 4), (1, 32))),
        "key_input": bell_draw(key_of[1], (BATCH, LENGTH, FEATURES), 1.0, 6.0, ((0, 4), (1, 32))),
        "value_input": bell_draw(key_of[2], (BATCH, LENGTH, FEATURES), 1.0, 6.0, ((0, 4), (1, 32))),
        "grad_output": bell_draw(key_of[3], (BATCH, LENGTH, OUT_COLS), 1.0, 6.0, ((0, 4), (1, 32))),
        "out_weight": bell_draw(key_of[4], (FEATURES, OUT_COLS), FEATURES ** -0.5, 0.125, ((0, 128),)),
        "norm_gain": jnp.clip(1.0 + 0.18 * jax.random.normal(key_of[5], (FEATURES,), jnp.float32), 0.1, 1.9),
    }


epsilon = 1e-06

def silu_slope(inputs):
    sigmoid_value = jax.nn.sigmoid(inputs)
    return sigmoid_value * (1.0 + inputs * (1.0 - sigmoid_value))

def causal_product(left, right):
    scores = jnp.einsum('ihd,jhd->hij', left.astype(jnp.float32), right.astype(jnp.float32))
    length_now = left.shape[0]
    causal = jnp.arange(length_now)[:, None] >= jnp.arange(length_now)[None, :]
    return jnp.where(causal[None], scores, 0.0)

def product(form, left, right):
    return jnp.einsum(form, left.astype(jnp.float32), right.astype(jnp.float32))

def one_sequence(pieces):
    query_input, key_input, value_input, grad_result, out_weight, norm_gain = pieces
    blocks = LENGTH // BLOCK
    query_raw = query_input.astype(jnp.float32)
    key_raw = key_input.astype(jnp.float32)
    feat_query = jax.nn.silu(query_raw).astype(jnp.bfloat16).reshape(blocks, BLOCK, HEADS, HEAD_DIM)
    feat_key = jax.nn.silu(key_raw).astype(jnp.bfloat16).reshape(blocks, BLOCK, HEADS, HEAD_DIM)
    value_blocks = value_input.reshape(blocks, BLOCK, HEADS, HEAD_DIM)
    zero_state = jnp.zeros((HEADS, HEAD_DIM, HEAD_DIM), jnp.float32)

    def forward_step(state, items):
        query_block, key_block, value_block = items
        state_low = state.astype(jnp.bfloat16)
        score_block = causal_product(query_block, key_block).astype(jnp.bfloat16)
        inside = product('hij,jhe->ihe', score_block, value_block)
        carried = product('ihd,hde->ihe', query_block, state_low)
        update = product('jhd,jhe->hde', key_block, value_block)
        return (state + update, (inside + carried, state_low))
    unused, (attention, prefix) = lax.scan(forward_step, zero_state, (feat_query, feat_key, value_blocks))
    attention = attention.reshape(LENGTH, FEATURES)
    radius = jnp.sqrt(lax.optimization_barrier(jnp.mean(attention * attention, axis=-1, keepdims=True)) + epsilon)
    normed = attention / radius
    mixed = (normed * norm_gain).astype(jnp.bfloat16)
    result = jnp.dot(mixed, out_weight, preferred_element_type=jnp.float32).astype(jnp.bfloat16)
    grad_mixed = jnp.dot(grad_result, out_weight.T, preferred_element_type=jnp.float32)
    grad_hat = grad_mixed * norm_gain
    grad_att = (grad_hat - normed * lax.optimization_barrier(jnp.mean(grad_hat * normed, axis=-1, keepdims=True))) / radius
    grad_att = grad_att.astype(jnp.bfloat16).reshape(blocks, BLOCK, HEADS, HEAD_DIM)

    def backward_step(later, items):
        query_block, key_block, value_block, grad_block, state_low = items
        later_low = later.astype(jnp.bfloat16)
        score_block = causal_product(query_block, key_block).astype(jnp.bfloat16)
        grad_scores = causal_product(grad_block, value_block).astype(jnp.bfloat16)
        grad_fq = product('hij,jhd->ihd', grad_scores, key_block) + product('ihe,hde->ihd', grad_block, state_low)
        grad_fk = product('hij,ihd->jhd', grad_scores, query_block) + product('jhe,hde->jhd', value_block, later_low)
        grad_fv = product('hij,ihe->jhe', score_block, grad_block) + product('jhd,hde->jhe', key_block, later_low)
        update = product('ihd,ihe->hde', query_block, grad_block)
        return (later + update, (grad_fq, grad_fk, grad_fv))
    unused, (grad_fq, grad_fk, grad_fv) = lax.scan(backward_step, zero_state, (feat_query, feat_key, value_blocks, grad_att, prefix), reverse=True)
    grad_query = (grad_fq.reshape(LENGTH, FEATURES) * silu_slope(query_raw)).astype(jnp.bfloat16)
    grad_key = (grad_fk.reshape(LENGTH, FEATURES) * silu_slope(key_raw)).astype(jnp.bfloat16)
    grad_value = grad_fv.reshape(LENGTH, FEATURES).astype(jnp.bfloat16)
    weight_term = jnp.dot(mixed.T, grad_result, preferred_element_type=jnp.float32)
    return (result, grad_query, grad_key, grad_value, weight_term)

def reference(query_input, key_input, value_input, grad_output, out_weight, norm_gain):

    def run(items):
        return one_sequence(items + (out_weight, norm_gain))
    result, grad_query, grad_key, grad_value, terms = lax.map(run, (query_input, key_input, value_input, grad_output))
    grad_weight = lax.optimization_barrier(jnp.sum(terms, axis=0))
    return (result, grad_query, grad_key, grad_value, grad_weight)
```

```python
import jax
import jax.numpy as jnp
from jax import lax
from jax.sharding import Mesh
from jax.sharding import PartitionSpec as P

HEADS = 16
HEAD_DIM = 128
BLOCK = 512
SEQ = ("seq_0", "seq_1", "seq_2")
SEQ_DP = ("seq_0", "seq_1", "seq_2", "dp")


epsilon = 1e-06


def scanned(block_state, reverse):
    peers = 1
    for axis in SEQ:
        peers *= lax.axis_size(axis)
    pieces = block_state.astype(jnp.bfloat16).reshape(peers, -1, HEAD_DIM)
    pieces = lax.all_to_all(pieces, SEQ, 0, 0, tiled=True)
    row = lax.broadcasted_iota(jnp.int32, (peers, peers), 0)
    col = lax.broadcasted_iota(jnp.int32, (peers, peers), 1)
    passed = (row < col) if reverse else (row > col)
    sums = jnp.einsum(
        "ij,jkl->ikl", passed.astype(jnp.bfloat16), pieces, preferred_element_type=jnp.float32
    )
    sums = lax.all_to_all(sums.astype(jnp.bfloat16), SEQ, 0, 0, tiled=True)
    return sums.reshape(block_state.shape)


def gradient_rows(mixed, grad_result):
    chips = lax.axis_size("seq_0") * lax.axis_size("seq_1")
    left = mixed.reshape(mixed.shape[0], chips, 2, -1)
    core = lax.axis_index("seq_2")
    mine = lax.dynamic_index_in_dim(left, core, 2, keepdims=False)
    other = lax.dynamic_index_in_dim(left, 1 - core, 2, keepdims=False)
    form = "tcr,tn->crn"
    sent = jnp.einsum(form, other, grad_result, preferred_element_type=jnp.float32)
    got = lax.ppermute(sent.astype(jnp.bfloat16), "seq_2", [(0, 1), (1, 0)])
    kept = jnp.einsum(form, mine, grad_result, preferred_element_type=jnp.float32)
    total = (kept + got.astype(jnp.float32)).astype(jnp.bfloat16)
    places = chips * lax.axis_size("dp")
    total = total.reshape(places, -1, total.shape[-1])
    total = lax.all_to_all(total, ("seq_0", "seq_1", "dp"), 0, 0, tiled=True)
    return jnp.sum(total.astype(jnp.float32), axis=0)


def silu_slope(inputs):
    sigmoid_value = jax.nn.sigmoid(inputs)
    return sigmoid_value * (1.0 + inputs * (1.0 - sigmoid_value))


def causal_product(left, right):
    scores = jnp.einsum("ihd,jhd->hij", left, right, preferred_element_type=jnp.float32)
    length_now = left.shape[0]
    causal = jnp.arange(length_now)[:, None] >= jnp.arange(length_now)[None, :]
    return jnp.where(causal[None], scores, 0.0)


def product(form, left, right):
    return jnp.einsum(form, left, right, preferred_element_type=jnp.float32)


def forward_parts(query_block, key_block, value_block, state_low):
    score_block = causal_product(query_block, key_block).astype(jnp.bfloat16)
    inside = product("hij,jhe->ihe", score_block, value_block)
    carried = product("ihd,hde->ihe", query_block, state_low)
    return (inside + carried, score_block)


def forward_only(items):
    return forward_parts(*items)[0]


def backward_core(
    query_block, key_block, value_block, grad_block, state_low, later_low, score_block
):
    grad_scores = causal_product(grad_block, value_block).astype(jnp.bfloat16)
    grad_fq = product("hij,jhd->ihd", grad_scores, key_block) + product(
        "ihe,hde->ihd", grad_block, state_low
    )
    grad_fk = product("hij,ihd->jhd", grad_scores, query_block) + product(
        "jhe,hde->jhd", value_block, later_low
    )
    grad_fv = product("hij,ihe->jhe", score_block, grad_block) + product(
        "jhd,hde->jhe", key_block, later_low
    )
    return (grad_fq, grad_fk, grad_fv)


def backward_again(items):
    query_block, key_block = (items[0], items[1])
    score_block = causal_product(query_block, key_block).astype(jnp.bfloat16)
    return backward_core(*items + (score_block,))


def shards(query_input, key_input, value_input, grad_output, out_weight, norm_gain):
    tokens = query_input.shape[1]
    feature_count = query_input.shape[2]
    blocks = tokens // BLOCK
    query_raw = query_input[0].astype(jnp.float32)
    key_raw = key_input[0].astype(jnp.float32)
    feat_query = jax.nn.silu(query_raw).astype(jnp.bfloat16).reshape(blocks, BLOCK, HEADS, HEAD_DIM)
    feat_key = jax.nn.silu(key_raw).astype(jnp.bfloat16).reshape(blocks, BLOCK, HEADS, HEAD_DIM)
    value_blocks = value_input[0].reshape(blocks, BLOCK, HEADS, HEAD_DIM)
    block_kv = product("bjhd,bjhe->bhde", feat_key, value_blocks)
    prefix = scanned(block_kv[0], False)[None]
    full_weight = lax.all_gather(out_weight, SEQ_DP, axis=0, tiled=True)
    attention = lax.map(forward_only, (feat_query, feat_key, value_blocks, prefix))
    attention = attention.reshape(tokens, feature_count)
    radius = jnp.sqrt(jnp.mean(attention * attention, axis=-1, keepdims=True) + epsilon)
    normed = attention / radius
    mixed = (normed * norm_gain).astype(jnp.bfloat16)
    result = jnp.dot(mixed, full_weight, preferred_element_type=jnp.float32).astype(jnp.bfloat16)
    grad_result = grad_output[0]
    grad_mixed = lax.dot_general(
        grad_result, full_weight, (((1,), (1,)), ((), ())), preferred_element_type=jnp.float32
    )
    grad_hat = grad_mixed * norm_gain
    grad_att = (grad_hat - normed * jnp.mean(grad_hat * normed, axis=-1, keepdims=True)) / radius
    grad_att = grad_att.astype(jnp.bfloat16).reshape(blocks, BLOCK, HEADS, HEAD_DIM)
    block_grad = product("bihd,bihe->bhde", feat_query, grad_att)
    later = scanned(block_grad[0], True)[None]
    grad_fq, grad_fk, grad_fv = lax.map(
        backward_again, (feat_query, feat_key, value_blocks, grad_att, prefix, later)
    )
    grad_query = (grad_fq.reshape(tokens, feature_count) * silu_slope(query_raw)).astype(
        jnp.bfloat16
    )
    grad_key = (grad_fk.reshape(tokens, feature_count) * silu_slope(key_raw)).astype(jnp.bfloat16)
    grad_value = grad_fv.reshape(tokens, feature_count).astype(jnp.bfloat16)
    grad_weight = gradient_rows(mixed, grad_result)
    return (result[None], grad_query[None], grad_key[None], grad_value[None], grad_weight)


def solution(mesh):
    torus = Mesh(mesh.devices.reshape(4, 4, 2, mesh.shape["dp"]), ("seq_0", "seq_1", "seq_2", "dp"))
    placed = (
        P("dp", SEQ, None),
        P("dp", SEQ, None),
        P("dp", SEQ, None),
        P("dp", SEQ, None),
        P(SEQ_DP, None),
        P(),
    )
    return jax.shard_map(
        shards,
        mesh=torus,
        in_specs=placed,
        out_specs=(
            P("dp", SEQ, None),
            P("dp", SEQ, None),
            P("dp", SEQ, None),
            P("dp", SEQ, None),
            P(SEQ_DP, None),
        ),
        check_vma=False,
    )
```

```python
import jax
import jax.numpy as jnp
from jax import lax
from jax.experimental import pallas as pl
from jax.experimental.pallas import tpu as pltpu
from jax.sharding import Mesh
from jax.sharding import PartitionSpec as P

HEADS = 16
HEAD_DIM = 128
BLOCK = 512
HALF = BLOCK // 2
PAIR = 2 * HEAD_DIM
FEATURES = HEADS * HEAD_DIM
ROWS = 128
SEQ = ("seq_0", "seq_1", "seq_2")
SEQ_DP = ("seq_0", "seq_1", "seq_2", "dp")
F32 = jnp.float32
BF16 = jnp.bfloat16


epsilon = 1e-06


def head(i):
    return slice(i * HEAD_DIM, (i + 1) * HEAD_DIM)


def dot_nn(left, right):
    return lax.dot_general(left, right, (((1,), (0,)), ((), ())), preferred_element_type=F32)


def dot_nt(left, right):
    return lax.dot_general(left, right, (((1,), (1,)), ((), ())), preferred_element_type=F32)


def dot_tn(left, right):
    return lax.dot_general(left, right, (((0,), (0,)), ((), ())), preferred_element_type=F32)


def silu_low(raw):
    wide = raw.astype(F32)
    return (wide * jax.nn.sigmoid(wide)).astype(BF16)


def silu_slope(raw):
    wide = raw.astype(F32)
    s = jax.nn.sigmoid(wide)
    return s * (1.0 + wide * (1.0 - s))


def causal(scores):
    row = lax.broadcasted_iota(jnp.int32, scores.shape, 0)
    col = lax.broadcasted_iota(jnp.int32, scores.shape, 1)
    return jnp.where(row >= col, scores, 0.0).astype(BF16)


def spec(shape, index):
    return pl.BlockSpec(shape, index)


def call(body, grid, in_specs, out_specs, out_shape, flops, moved, scratch=(), name=None):
    return pl.pallas_call(
        body,
        grid=grid,
        in_specs=in_specs,
        out_specs=out_specs,
        out_shape=out_shape,
        scratch_shapes=scratch,
        compiler_params=pltpu.CompilerParams(vmem_limit_bytes=48 * 1024 * 1024),
        cost_estimate=pl.CostEstimate(flops=flops, bytes_accessed=moved, transcendentals=0),
        name=name,
    )


PAIR_SPEC = spec((BLOCK, PAIR), lambda i: (0, i))
STATE_SPEC = spec((2, HEAD_DIM, HEAD_DIM), lambda i: (i, 0, 0))
WIDE_LOW = jax.ShapeDtypeStruct((BLOCK, FEATURES), BF16)
WIDE = jax.ShapeDtypeStruct((BLOCK, FEATURES), F32)
STATE_LOW = jax.ShapeDtypeStruct((HEADS, HEAD_DIM, HEAD_DIM), BF16)
MIB = 1 << 20


def states_body(key, value, feat_key, state):
    for i in range(2):
        low = silu_low(key[:, head(i)])
        feat_key[:, head(i)] = low
        state[i] = dot_tn(low, value[:, head(i)]).astype(BF16)


def block_states(key, value):
    return call(
        states_body,
        (HEADS // 2,),
        [PAIR_SPEC, PAIR_SPEC],
        [PAIR_SPEC, STATE_SPEC],
        [WIDE_LOW, STATE_LOW],
        1 << 29,
        7 * MIB,
        name="block_states",
    )(key, value)


def inside_body(query, feat_key, value, feat_query, inside):
    for i in range(2):
        low = silu_low(query[:, head(i)])
        feat_query[:, head(i)] = low
        keys = feat_key[:, head(i)]
        values = value[:, head(i)]
        first = causal(dot_nt(low[:HALF], keys[:HALF]))
        below = dot_nt(low[HALF:], keys[:HALF]).astype(BF16)
        second = causal(dot_nt(low[HALF:], keys[HALF:]))
        inside[:HALF, head(i)] = dot_nn(first, values[:HALF])
        inside[HALF:, head(i)] = dot_nn(below, values[:HALF]) + dot_nn(second, values[HALF:])


def inside_blocks(query, feat_key, value):
    return call(
        inside_body,
        (HEADS // 2,),
        [PAIR_SPEC] * 3,
        [PAIR_SPEC] * 2,
        [WIDE_LOW, WIDE],
        1 << 32,
        12 * MIB,
        name="inside_blocks",
    )(query, feat_key, value)


def scan_body(reverse, pieces, sums):
    peers = pieces.shape[0]
    total = jnp.zeros(pieces.shape[1:], F32)
    for k in reversed(range(peers)) if reverse else range(peers):
        sums[k] = total.astype(BF16)
        total = total + pieces[k].astype(F32)


def exclusive_sums(pieces, reverse):
    peers, rows, lanes = pieces.shape
    part = spec((peers, rows // 2, lanes), lambda i: (0, i, 0))
    return call(
        lambda a, b: scan_body(reverse, a, b),
        (2,),
        [part],
        part,
        jax.ShapeDtypeStruct(pieces.shape, BF16),
        1 << 23,
        MIB,
        name="exclusive_sums",
    )(pieces)


def scanned(block_state, reverse):
    peers = 1
    for axis in SEQ:
        peers *= lax.axis_size(axis)
    pieces = block_state.reshape(peers, -1, HEAD_DIM)
    pieces = lax.all_to_all(pieces, SEQ, 0, 0, tiled=True)
    sums = exclusive_sums(pieces, reverse)
    sums = lax.all_to_all(sums, SEQ, 0, 0, tiled=True)
    return sums.reshape(block_state.shape)


ROW_SPEC = spec((ROWS, FEATURES), lambda i: (i, 0))
EDGE_SPEC = spec((ROWS, HEAD_DIM), lambda i: (i, 0))
GAIN_SPEC = spec((1, FEATURES), lambda i: (0, 0))
ALL_STATES = spec((HEADS, HEAD_DIM, HEAD_DIM), lambda i: (0, 0, 0))
SPLIT_SPEC = spec((2, ROWS, FEATURES // 2), lambda i: (0, i, 0))


def attend_body(inside, feat_query, state, gain, mixed, split, normed, inverse):
    squares = jnp.zeros((ROWS, HEAD_DIM), F32)
    for i in range(HEADS):
        attention = inside[:, head(i)] + dot_nn(feat_query[:, head(i)], state[i])
        normed[:, head(i)] = attention
        squares = squares + attention * attention
    radius = jnp.sqrt(jnp.sum(squares, axis=1, keepdims=True) / FEATURES + epsilon)
    scale = 1.0 / radius
    inverse[...] = jnp.broadcast_to(scale, inverse.shape)
    part = HEAD_DIM // 2
    for i in range(0, HEADS, 2):
        lows = []
        for j in (i, i + 1):
            value = normed[:, head(j)] * scale
            normed[:, head(j)] = value
            low = (value * gain[:, head(j)]).astype(BF16)
            mixed[:, head(j)] = low
            lows.append(low)
        at = head(i // 2)
        split[0, :, at] = jnp.concatenate([lows[0][:, :part], lows[1][:, :part]], axis=1)
        split[1, :, at] = jnp.concatenate([lows[0][:, part:], lows[1][:, part:]], axis=1)


def attend(inside, feat_query, state, gain):
    return call(
        attend_body,
        (BLOCK // ROWS,),
        [ROW_SPEC, ROW_SPEC, ALL_STATES, GAIN_SPEC],
        [ROW_SPEC, SPLIT_SPEC, ROW_SPEC, EDGE_SPEC],
        [
            WIDE_LOW,
            jax.ShapeDtypeStruct((2, BLOCK, FEATURES // 2), BF16),
            WIDE,
            jax.ShapeDtypeStruct((BLOCK, HEAD_DIM), F32),
        ],
        1 << 29,
        15 * MIB,
        name="attend",
    )(inside, feat_query, state, gain)


def norm_back_body(grad_mixed, normed, inverse, gain, feat_query, grad_att, state, sums):
    step = pl.program_id(0)
    products = jnp.zeros((ROWS, HEAD_DIM), F32)
    for i in range(HEADS):
        hat = grad_mixed[:, head(i)] * gain[:, head(i)]
        products = products + hat * normed[:, head(i)]
    mean = jnp.sum(products, axis=1, keepdims=True) / FEATURES
    scale = inverse[:, :1]
    for i in range(HEADS):
        hat = grad_mixed[:, head(i)] * gain[:, head(i)]
        low = ((hat - normed[:, head(i)] * mean) * scale).astype(BF16)
        grad_att[:, head(i)] = low
        update = dot_tn(feat_query[:, head(i)], low)

        @pl.when(step == 0)
        def _():
            sums[i] = update

        @pl.when(step > 0)
        def _():
            sums[i] = sums[i] + update

    @pl.when(step == pl.num_programs(0) - 1)
    def _():
        state[...] = sums[...].astype(BF16)


def norm_back(grad_mixed, normed, inverse, gain, feat_query):
    return call(
        norm_back_body,
        (BLOCK // ROWS,),
        [ROW_SPEC, ROW_SPEC, EDGE_SPEC, GAIN_SPEC, ROW_SPEC],
        [ROW_SPEC, ALL_STATES],
        [WIDE_LOW, STATE_LOW],
        1 << 29,
        13 * MIB,
        scratch=[pltpu.VMEM((HEADS, HEAD_DIM, HEAD_DIM), F32)],
        name="norm_back",
    )(grad_mixed, normed, inverse, gain, feat_query)


def back_body(query, feat_query, feat_key, value, grad, state, grad_query, part_key, part_value):
    for i in range(2):
        at = head(i)
        q0, q1 = feat_query[:HALF, at], feat_query[HALF:, at]
        k0, k1 = feat_key[:HALF, at], feat_key[HALF:, at]
        v0, v1 = value[:HALF, at], value[HALF:, at]
        g0, g1 = grad[:HALF, at], grad[HALF:, at]
        s00 = causal(dot_nt(q0, k0))
        s10 = dot_nt(q1, k0).astype(BF16)
        s11 = causal(dot_nt(q1, k1))
        part_value[:HALF, at] = dot_tn(s00, g0) + dot_tn(s10, g1)
        part_value[HALF:, at] = dot_tn(s11, g1)
        d00 = causal(dot_nt(g0, v0))
        d10 = dot_nt(g1, v0).astype(BF16)
        d11 = causal(dot_nt(g1, v1))
        part_key[:HALF, at] = dot_tn(d00, q0) + dot_tn(d10, q1)
        part_key[HALF:, at] = dot_tn(d11, q1)
        fq0 = dot_nn(d00, k0) + dot_nt(g0, state[i])
        fq1 = dot_nn(d10, k0) + dot_nn(d11, k1) + dot_nt(g1, state[i])
        grad_query[:HALF, at] = (fq0 * silu_slope(query[:HALF, at])).astype(BF16)
        grad_query[HALF:, at] = (fq1 * silu_slope(query[HALF:, at])).astype(BF16)


def back_inside(query, feat_query, feat_key, value, grad, state):
    return call(
        back_body,
        (HEADS // 2,),
        [PAIR_SPEC] * 5 + [STATE_SPEC],
        [PAIR_SPEC] * 3,
        [WIDE_LOW, WIDE, WIDE],
        3 << 32,
        20 * MIB,
        name="back_inside",
    )(query, feat_query, feat_key, value, grad, state)


def finish_body(key, feat_key, value, part_key, part_value, later, grad_key, grad_value):
    for i in range(2):
        at = head(i)
        fk = part_key[:, at] + dot_nt(value[:, at], later[i])
        grad_key[:, at] = (fk * silu_slope(key[:, at])).astype(BF16)
        grad_value[:, at] = (part_value[:, at] + dot_nn(feat_key[:, at], later[i])).astype(BF16)


def finish(key, feat_key, value, part_key, part_value, later):
    return call(
        finish_body,
        (HEADS // 2,),
        [PAIR_SPEC] * 5 + [STATE_SPEC],
        [PAIR_SPEC] * 2,
        [WIDE_LOW, WIDE_LOW],
        1 << 30,
        18 * MIB,
        name="finish",
    )(key, feat_key, value, part_key, part_value, later)


def gradient_rows(split, grad_result):
    chips = lax.axis_size("seq_0") * lax.axis_size("seq_1")
    core = lax.axis_index("seq_2")
    mine = lax.dynamic_index_in_dim(split, core, 0, keepdims=False)
    other = lax.dynamic_index_in_dim(split, 1 - core, 0, keepdims=False)
    sent = dot_tn(other, grad_result).astype(BF16)
    got = lax.ppermute(sent, "seq_2", [(0, 1), (1, 0)])
    kept = dot_tn(mine, grad_result)
    total = (kept + got.astype(F32)).astype(BF16)
    places = chips * lax.axis_size("dp")
    total = total.reshape(places, -1, total.shape[-1])
    total = lax.all_to_all(total, ("seq_0", "seq_1", "dp"), 0, 0, tiled=True)
    return jnp.sum(total.astype(F32), axis=0)


def shards(query_input, key_input, value_input, grad_output, out_weight, norm_gain):
    query, key, value, grad_result = query_input[0], key_input[0], value_input[0], grad_output[0]
    gain = norm_gain.reshape(1, FEATURES)
    full_weight = lax.all_gather(out_weight, SEQ_DP, axis=0, tiled=True)
    feat_key, block_kv = block_states(key, value)
    prefix = scanned(block_kv, False)
    feat_query, inside = inside_blocks(query, feat_key, value)
    mixed, split, normed, inverse = attend(inside, feat_query, prefix, gain)
    grad_weight = gradient_rows(split, grad_result)
    grad_mixed = dot_nt(grad_result, full_weight)
    grad_att, block_grad = norm_back(grad_mixed, normed, inverse, gain, feat_query)
    later = scanned(block_grad, True)
    result = dot_nn(mixed, full_weight).astype(BF16)
    grad_query, part_key, part_value = back_inside(
        query, feat_query, feat_key, value, grad_att, prefix
    )
    grad_key, grad_value = finish(key, feat_key, value, part_key, part_value, later)
    return (result[None], grad_query[None], grad_key[None], grad_value[None], grad_weight)


def solution(mesh):
    torus = Mesh(mesh.devices.reshape(4, 4, 2, mesh.shape["dp"]), ("seq_0", "seq_1", "seq_2", "dp"))
    placed = (
        P("dp", SEQ, None),
        P("dp", SEQ, None),
        P("dp", SEQ, None),
        P("dp", SEQ, None),
        P(SEQ_DP, None),
        P(),
    )
    return jax.shard_map(
        shards,
        mesh=torus,
        in_specs=placed,
        out_specs=(
            P("dp", SEQ, None),
            P("dp", SEQ, None),
            P("dp", SEQ, None),
            P("dp", SEQ, None),
            P(SEQ_DP, None),
        ),
        check_vma=False,
    )
```

```python
import jax
import jax.numpy as jnp
from jax import lax
from jax.experimental import pallas as pl
from jax.experimental.pallas import tpu as pltpu
from jax.sharding import Mesh
from jax.sharding import PartitionSpec as P


HEADS = 16
HEAD_DIM = 128
BLOCK = 512
HALF = BLOCK // 2
GROUP = 4
PAIR = GROUP * HEAD_DIM
FEATURES = HEADS * HEAD_DIM
ROWS = 128
SEQ = ("seq_0", "seq_1", "seq_2")
SEQ_DP = ("seq_0", "seq_1", "seq_2", "dp")
F32 = jnp.float32
BF16 = jnp.bfloat16


epsilon = 1e-06


def head(i):
    return slice(i * HEAD_DIM, (i + 1) * HEAD_DIM)


def dot_nn(left, right):
    return lax.dot_general(left, right, (((1,), (0,)), ((), ())), preferred_element_type=F32)


def dot_nt(left, right):
    return lax.dot_general(left, right, (((1,), (1,)), ((), ())), preferred_element_type=F32)


def dot_tn(left, right):
    return lax.dot_general(left, right, (((0,), (0,)), ((), ())), preferred_element_type=F32)


def silu_low(raw):
    wide = raw.astype(F32)
    return (wide * jax.nn.sigmoid(wide)).astype(BF16)


def silu_slope(raw):
    wide = raw.astype(F32)
    s = jax.nn.sigmoid(wide)
    return s * (1.0 + wide * (1.0 - s))


def causal(scores):
    row = lax.broadcasted_iota(jnp.int32, scores.shape, 0)
    col = lax.broadcasted_iota(jnp.int32, scores.shape, 1)
    return jnp.where(row >= col, scores, 0.0).astype(BF16)


def spec(shape, index):
    return pl.BlockSpec(shape, index)


def call(body, grid, in_specs, out_specs, out_shape, flops, moved, scratch=()):
    return pl.pallas_call(
        body,
        grid=grid,
        in_specs=in_specs,
        out_specs=out_specs,
        out_shape=out_shape,
        scratch_shapes=scratch,
        compiler_params=pltpu.CompilerParams(vmem_limit_bytes=60 * 1024 * 1024),
        cost_estimate=pl.CostEstimate(flops=flops, bytes_accessed=moved, transcendentals=0),
    )


PAIR_SPEC = spec((BLOCK, PAIR), lambda i: (0, i))
STATE_SPEC = spec((GROUP, HEAD_DIM, HEAD_DIM), lambda i: (i, 0, 0))
WIDE_LOW = jax.ShapeDtypeStruct((BLOCK, FEATURES), BF16)
WIDE = jax.ShapeDtypeStruct((BLOCK, FEATURES), F32)
STATE_LOW = jax.ShapeDtypeStruct((HEADS, HEAD_DIM, HEAD_DIM), BF16)
MIB = 1 << 20


def states_body(key, value, feat_key, state):
    for i in range(GROUP):
        low = silu_low(key[:, head(i)])
        feat_key[:, head(i)] = low
        state[i] = dot_tn(low, value[:, head(i)]).astype(BF16)


def block_states(key, value):
    return call(
        states_body,
        (HEADS // GROUP,),
        [PAIR_SPEC, PAIR_SPEC],
        [PAIR_SPEC, STATE_SPEC],
        [WIDE_LOW, STATE_LOW],
        1 << 29,
        7 * MIB,
    )(key, value)


def inside_body(query, feat_key, value, feat_query, inside):
    for i in range(GROUP):
        low = silu_low(query[:, head(i)])
        feat_query[:, head(i)] = low
        keys = feat_key[:, head(i)]
        values = value[:, head(i)]
        first = causal(dot_nt(low[:HALF], keys[:HALF]))
        below = dot_nt(low[HALF:], keys[:HALF]).astype(BF16)
        second = causal(dot_nt(low[HALF:], keys[HALF:]))
        inside[:HALF, head(i)] = dot_nn(first, values[:HALF])
        inside[HALF:, head(i)] = dot_nn(below, values[:HALF]) + dot_nn(second, values[HALF:])


def inside_blocks(query, feat_key, value):
    return call(
        inside_body,
        (HEADS // GROUP,),
        [PAIR_SPEC] * 3,
        [PAIR_SPEC] * 2,
        [WIDE_LOW, WIDE],
        1 << 32,
        12 * MIB,
    )(query, feat_key, value)


def scan_body(reverse, pieces, sums):
    peers = pieces.shape[0]
    total = jnp.zeros(pieces.shape[1:], F32)
    for k in reversed(range(peers)) if reverse else range(peers):
        sums[k] = total.astype(BF16)
        total = total + pieces[k].astype(F32)


def exclusive_sums(pieces, reverse):
    peers, rows, lanes = pieces.shape
    part = spec((peers, rows // 2, lanes), lambda i: (0, i, 0))
    return call(
        lambda a, b: scan_body(reverse, a, b),
        (2,),
        [part],
        part,
        jax.ShapeDtypeStruct(pieces.shape, BF16),
        1 << 23,
        MIB,
    )(pieces)


def scanned(block_state, reverse):
    peers = 1
    for axis in SEQ:
        peers *= lax.axis_size(axis)
    pieces = block_state.reshape(peers, -1, HEAD_DIM)
    pieces = lax.all_to_all(pieces, SEQ, 0, 0, tiled=True)
    sums = exclusive_sums(pieces, reverse)
    sums = lax.all_to_all(sums, SEQ, 0, 0, tiled=True)
    return sums.reshape(block_state.shape)


ROW_SPEC = spec((ROWS, FEATURES), lambda i: (i, 0))
EDGE_SPEC = spec((ROWS, HEAD_DIM), lambda i: (i, 0))
GAIN_SPEC = spec((1, FEATURES), lambda i: (0, 0))
ALL_STATES = spec((HEADS, HEAD_DIM, HEAD_DIM), lambda i: (0, 0, 0))
SPLIT_SPEC = spec((2, ROWS, FEATURES // 2), lambda i: (0, i, 0))


def attend_body(inside, feat_query, state, gain, mixed, split, normed, inverse):
    squares = jnp.zeros((ROWS, HEAD_DIM), F32)
    for i in range(HEADS):
        attention = inside[:, head(i)] + dot_nn(feat_query[:, head(i)], state[i])
        normed[:, head(i)] = attention
        squares = squares + attention * attention
    radius = jnp.sqrt(jnp.sum(squares, axis=1, keepdims=True) / FEATURES + epsilon)
    scale = 1.0 / radius
    inverse[...] = jnp.broadcast_to(scale, inverse.shape)
    part = HEAD_DIM // 2
    for i in range(0, HEADS, 2):
        lows = []
        for j in (i, i + 1):
            value = normed[:, head(j)] * scale
            normed[:, head(j)] = value
            low = (value * gain[:, head(j)]).astype(BF16)
            mixed[:, head(j)] = low
            lows.append(low)
        at = head(i // 2)
        split[0, :, at] = jnp.concatenate([lows[0][:, :part], lows[1][:, :part]], axis=1)
        split[1, :, at] = jnp.concatenate([lows[0][:, part:], lows[1][:, part:]], axis=1)


def attend(inside, feat_query, state, gain):
    return call(
        attend_body,
        (BLOCK // ROWS,),
        [ROW_SPEC, ROW_SPEC, ALL_STATES, GAIN_SPEC],
        [ROW_SPEC, SPLIT_SPEC, ROW_SPEC, EDGE_SPEC],
        [
            WIDE_LOW,
            jax.ShapeDtypeStruct((2, BLOCK, FEATURES // 2), BF16),
            WIDE,
            jax.ShapeDtypeStruct((BLOCK, HEAD_DIM), F32),
        ],
        1 << 29,
        15 * MIB,
    )(inside, feat_query, state, gain)


CHUNK = 2 * HEAD_DIM
CHUNKS = FEATURES // CHUNK


def norm_back_body(
    grad, weight, normed, inverse, gain, feat_query, grad_att, state, hats, norms, feats, products
):
    step = pl.program_id(0)

    @pl.when(step == 0)
    def _():
        products[...] = jnp.zeros_like(products)

    hat = dot_nt(grad[...], weight[...]) * gain[...]
    product = hat * normed[...]
    products[...] += product[:, :HEAD_DIM] + product[:, HEAD_DIM:]
    hats[step] = hat
    norms[step] = normed[...]
    feats[step] = feat_query[...]

    @pl.when(step == CHUNKS - 1)
    def _():
        mean = jnp.sum(products[...], axis=1, keepdims=True) / FEATURES
        scale = inverse[:, :1]
        for i in range(HEADS):
            c, at = i // 2, head(i % 2)
            low = ((hats[c, :, at] - norms[c, :, at] * mean) * scale).astype(BF16)
            grad_att[:, head(i)] = low
            state[i] = dot_tn(feats[c, :, at], low).astype(BF16)


def norm_back(grad_result, weight, normed, inverse, gain, feat_query):
    part = spec((BLOCK, CHUNK), lambda i: (0, i))
    whole = spec((BLOCK, FEATURES), lambda i: (0, 0))
    return call(
        norm_back_body,
        (CHUNKS,),
        [
            whole,
            spec((CHUNK, FEATURES), lambda i: (i, 0)),
            part,
            spec((BLOCK, HEAD_DIM), lambda i: (0, 0)),
            spec((1, CHUNK), lambda i: (0, i)),
            part,
        ],
        [whole, ALL_STATES],
        [WIDE_LOW, STATE_LOW],
        5 << 30,
        18 * MIB,
        scratch=[
            pltpu.VMEM((CHUNKS, BLOCK, CHUNK), F32),
            pltpu.VMEM((CHUNKS, BLOCK, CHUNK), F32),
            pltpu.VMEM((CHUNKS, BLOCK, CHUNK), BF16),
            pltpu.VMEM((BLOCK, HEAD_DIM), F32),
        ],
    )(grad_result, weight, normed, inverse, gain, feat_query)


def back_body(query, feat_query, feat_key, value, grad, state, grad_query, part_key, part_value):
    for i in range(GROUP):
        at = head(i)
        q0, q1 = feat_query[:HALF, at], feat_query[HALF:, at]
        k0, k1 = feat_key[:HALF, at], feat_key[HALF:, at]
        v0, v1 = value[:HALF, at], value[HALF:, at]
        g0, g1 = grad[:HALF, at], grad[HALF:, at]
        s00 = causal(dot_nt(q0, k0))
        s10 = dot_nt(q1, k0).astype(BF16)
        s11 = causal(dot_nt(q1, k1))
        part_value[:HALF, at] = dot_tn(s00, g0) + dot_tn(s10, g1)
        part_value[HALF:, at] = dot_tn(s11, g1)
        d00 = causal(dot_nt(g0, v0))
        d10 = dot_nt(g1, v0).astype(BF16)
        d11 = causal(dot_nt(g1, v1))
        part_key[:HALF, at] = dot_tn(d00, q0) + dot_tn(d10, q1)
        part_key[HALF:, at] = dot_tn(d11, q1)
        fq0 = dot_nn(d00, k0) + dot_nt(g0, state[i])
        fq1 = dot_nn(d10, k0) + dot_nn(d11, k1) + dot_nt(g1, state[i])
        grad_query[:HALF, at] = (fq0 * silu_slope(query[:HALF, at])).astype(BF16)
        grad_query[HALF:, at] = (fq1 * silu_slope(query[HALF:, at])).astype(BF16)


def back_inside(query, feat_query, feat_key, value, grad, state):
    return call(
        back_body,
        (HEADS // GROUP,),
        [PAIR_SPEC] * 5 + [STATE_SPEC],
        [PAIR_SPEC] * 3,
        [WIDE_LOW, WIDE, WIDE],
        3 << 32,
        20 * MIB,
    )(query, feat_query, feat_key, value, grad, state)


def finish_body(key, feat_key, value, part_key, part_value, later, grad_key, grad_value):
    for i in range(GROUP):
        at = head(i)
        fk = part_key[:, at] + dot_nt(value[:, at], later[i])
        grad_key[:, at] = (fk * silu_slope(key[:, at])).astype(BF16)
        grad_value[:, at] = (part_value[:, at] + dot_nn(feat_key[:, at], later[i])).astype(BF16)


def finish(key, feat_key, value, part_key, part_value, later):
    return call(
        finish_body,
        (HEADS // GROUP,),
        [PAIR_SPEC] * 5 + [STATE_SPEC],
        [PAIR_SPEC] * 2,
        [WIDE_LOW, WIDE_LOW],
        1 << 30,
        18 * MIB,
    )(key, feat_key, value, part_key, part_value, later)


COLORS = 4
WIDTH = FEATURES // COLORS
SLAB = 16
PLACES = 64
CYCLES = (((0, 1), (1, 0), (2, 3), (3, 2)), ((0, 3), (3, 0), (1, 2), (2, 1)))


def on_ring(low, high):
    return low + high * (3 - 2 * low)


def my_bits(axis):
    at = lax.axis_index(axis)
    high = (at >= 2).astype(jnp.int32)
    low = ((at == 1) | (at == 2)).astype(jnp.int32)
    return (low, high)


def hop(sent, axis, which):
    return lax.ppermute(sent, axis, CYCLES[which])


def product_body(place, left, right, out):
    out[...] = dot_tn(left[0], right[...]).astype(BF16)


def first_body(color, place, left, right, got, kept, sent, acc):
    acc[...] = (dot_tn(left[0], right[...]) + got[...].astype(F32)).astype(BF16)
    bit = place[2 + color]
    for side, out in ((bit, kept), (1 - bit, sent)):
        for s in range(PLACES // 2):
            other, rest, z = s // 16, (s // 4) % 4, s % 4
            z = on_ring(z // 2, z % 2)
            far = on_ring(rest // 2, rest % 2)
            near = on_ring(side, other) if color % 2 == 0 else on_ring(other, side)
            y, x = (far, near) if color < 2 else (near, far)
            at = pl.multiple_of((y * 16 + z * 4 + x) * SLAB, SLAB)
            out[s * SLAB : (s + 1) * SLAB] = acc[pl.ds(at, SLAB)]


def gradient_rows(split, grad_result):
    core = lax.axis_index("seq_2")
    xs, ys, zs = my_bits("dp"), my_bits("seq_0"), my_bits("seq_1")
    place = jnp.stack([core, 1 - core, xs[0], xs[1], ys[0], ys[1]]).astype(jnp.int32)
    half = FEATURES // 2

    def grid_spec(which, color, more, outs):
        return pltpu.PrefetchScalarGridSpec(
            num_scalar_prefetch=1,
            grid=(1,),
            in_specs=[
                pl.BlockSpec((1, BLOCK, half), lambda i, p: (p[which], 0, 0)),
                pl.BlockSpec((BLOCK, WIDTH), lambda i, p: (0, color)),
            ]
            + more,
            out_specs=outs,
            scratch_shapes=[pltpu.VMEM((half, WIDTH), BF16)] if more else [],
        )

    whole = pl.BlockSpec((half, WIDTH), lambda i, p: (0, 0))
    part = pl.BlockSpec((half // 2, WIDTH), lambda i, p: (0, 0))
    params = pltpu.CompilerParams(vmem_limit_bytes=32 * MIB)
    cost = pl.CostEstimate(flops=1 << 30, bytes_accessed=4 * MIB, transcendentals=0)

    gots = []
    for color in range(COLORS):
        sent = pl.pallas_call(
            product_body,
            grid_spec=grid_spec(1, color, [], whole),
            out_shape=jax.ShapeDtypeStruct((half, WIDTH), BF16),
            compiler_params=params,
            cost_estimate=cost,
            name="pair_product",
        )(place, split, grad_result)
        gots.append(lax.ppermute(sent, "seq_2", [(0, 1), (1, 0)]))
    order = ((xs, "dp"), (ys, "seq_0"))
    keeps = []
    for color in range(COLORS):
        kept, sent = pl.pallas_call(
            lambda *refs, color=color: first_body(color, *refs),
            grid_spec=grid_spec(0, color, [whole], [part, part]),
            out_shape=[jax.ShapeDtypeStruct((half // 2, WIDTH), BF16)] * 2,
            compiler_params=params,
            cost_estimate=cost,
            name="first_halves",
        )(place, split, grad_result, gots[color])
        keeps.append((kept, hop(sent, order[color // 2][1], color % 2)))

    def halves(total, bit, axis):
        count = total.shape[axis] // 2
        kept = lax.dynamic_slice_in_dim(total, bit * count, count, axis)
        sent = lax.dynamic_slice_in_dim(total, (1 - bit) * count, count, axis)
        return (kept, sent)

    def add(kept, got):
        return (kept.astype(F32) + got.astype(F32)).astype(BF16)

    seconds = []
    for color, (kept, got) in enumerate(keeps):
        bits, axis = order[color // 2]
        which = 1 - color % 2
        kept, sent = halves(add(kept, got), bits[which], 0)
        seconds.append((kept, hop(sent, axis, which)))
    joined = []
    for near in range(2):
        bits, axis = order[1 - near]
        total = jnp.stack([add(*seconds[2 * near]), add(*seconds[2 * near + 1])])
        for which in range(2):
            kept, sent = halves(total, bits[which], 1)
            total = add(kept, hop(sent, axis, which))
        joined.append(total)
    total = jnp.concatenate(joined, axis=0)
    kept, sent = halves(total, zs[0], 1)
    total = add(kept, hop(sent, "seq_1", 0))
    kept, sent = halves(total, zs[1], 1)
    total = kept.astype(F32) + hop(sent, "seq_1", 1).astype(F32)
    return jnp.concatenate([total[c] for c in range(COLORS)], axis=1)


def layer(query_input, key_input, value_input, grad_output, out_weight, norm_gain):
    query, key, value, grad_result = query_input[0], key_input[0], value_input[0], grad_output[0]
    gain = norm_gain.reshape(1, FEATURES)
    full_weight = lax.all_gather(out_weight, SEQ_DP, axis=0, tiled=True)
    feat_key, block_kv = block_states(key, value)
    prefix = scanned(block_kv, False)
    feat_query, inside = inside_blocks(query, feat_key, value)
    mixed, split, normed, inverse = attend(inside, feat_query, prefix, gain)
    grad_weight = gradient_rows(split, grad_result)
    grad_att, block_grad = norm_back(
        grad_result, full_weight, normed, inverse, gain, feat_query
    )
    later = scanned(block_grad, True)
    result = dot_nn(mixed, full_weight).astype(BF16)
    grad_query, part_key, part_value = back_inside(
        query, feat_query, feat_key, value, grad_att, prefix
    )
    grad_key, grad_value = finish(key, feat_key, value, part_key, part_value, later)
    return (result[None], grad_query[None], grad_key[None], grad_value[None], grad_weight)


def solution(mesh):
    torus = Mesh(mesh.devices.reshape(4, 4, 2, mesh.shape["dp"]), ("seq_0", "seq_1", "seq_2", "dp"))
    placed = (
        P("dp", SEQ, None),
        P("dp", SEQ, None),
        P("dp", SEQ, None),
        P("dp", SEQ, None),
        P(SEQ_DP, None),
        P(),
    )
    return jax.shard_map(
        layer,
        mesh=torus,
        in_specs=placed,
        out_specs=(
            P("dp", SEQ, None),
            P("dp", SEQ, None),
            P("dp", SEQ, None),
            P("dp", SEQ, None),
            P(SEQ_DP, None),
        ),
        check_vma=False,
    )
```

```python
import jax
import jax.numpy as jnp
from jax import lax
from jax.experimental import pallas as pl
from jax.experimental.pallas import tpu as pltpu
from jax.sharding import Mesh
from jax.sharding import PartitionSpec as P


HEADS = 16
HEAD_DIM = 128
BLOCK = 512
HALF = BLOCK // 2
GROUP = 4
PAIR = GROUP * HEAD_DIM
FEATURES = HEADS * HEAD_DIM
ROWS = 128
SEQ = ("seq_0", "seq_1", "seq_2")
SEQ_DP = ("seq_0", "seq_1", "seq_2", "dp")
F32 = jnp.float32
BF16 = jnp.bfloat16


epsilon = 1e-06


def head(i):
    return slice(i * HEAD_DIM, (i + 1) * HEAD_DIM)


def dot_nn(left, right):
    return lax.dot_general(left, right, (((1,), (0,)), ((), ())), preferred_element_type=F32)


def dot_nt(left, right):
    return lax.dot_general(left, right, (((1,), (1,)), ((), ())), preferred_element_type=F32)


def dot_tn(left, right):
    return lax.dot_general(left, right, (((0,), (0,)), ((), ())), preferred_element_type=F32)


def silu_low(raw):
    wide = raw.astype(F32)
    return (wide * jax.nn.sigmoid(wide)).astype(BF16)


def silu_slope(raw):
    wide = raw.astype(F32)
    s = jax.nn.sigmoid(wide)
    return s * (1.0 + wide * (1.0 - s))


def causal(scores):
    row = lax.broadcasted_iota(jnp.int32, scores.shape, 0)
    col = lax.broadcasted_iota(jnp.int32, scores.shape, 1)
    return jnp.where(row >= col, scores, 0.0).astype(BF16)


def spec(shape, index):
    return pl.BlockSpec(shape, index)


def call(body, grid, in_specs, out_specs, out_shape, flops, moved, scratch=()):
    return pl.pallas_call(
        body,
        grid=grid,
        in_specs=in_specs,
        out_specs=out_specs,
        out_shape=out_shape,
        scratch_shapes=scratch,
        compiler_params=pltpu.CompilerParams(vmem_limit_bytes=60 * 1024 * 1024),
        cost_estimate=pl.CostEstimate(flops=flops, bytes_accessed=moved, transcendentals=0),
    )


COLORS = 4
WIDTH = FEATURES // COLORS
SLAB = 16
PLACES = 64
CYCLES = (((0, 1), (1, 0), (2, 3), (3, 2)), ((0, 3), (3, 0), (1, 2), (2, 1)))
PAIR_SPEC = spec((BLOCK, PAIR), lambda i: (0, i))
STATE_SPEC = spec((GROUP, HEAD_DIM, HEAD_DIM), lambda i: (i, 0, 0))
WIDE_LOW = jax.ShapeDtypeStruct((BLOCK, FEATURES), BF16)
WIDE = jax.ShapeDtypeStruct((BLOCK, FEATURES), F32)
STATE_LOW = jax.ShapeDtypeStruct((HEADS, HEAD_DIM, HEAD_DIM), BF16)
MIB = 1 << 20


def states_body(key, value, feat_key, state):
    for i in range(GROUP):
        low = silu_low(key[:, head(i)])
        feat_key[:, head(i)] = low
        state[i] = dot_tn(low, value[:, head(i)]).astype(BF16)


def block_states(key, value):
    return call(
        states_body,
        (HEADS // GROUP,),
        [PAIR_SPEC, PAIR_SPEC],
        [PAIR_SPEC, STATE_SPEC],
        [WIDE_LOW, STATE_LOW],
        1 << 29,
        7 * MIB,
    )(key, value)


def inside_body(query, feat_key, value, feat_query, inside):
    for i in range(GROUP):
        low = silu_low(query[:, head(i)])
        feat_query[:, head(i)] = low
        keys = feat_key[:, head(i)]
        values = value[:, head(i)]
        first = causal(dot_nt(low[:HALF], keys[:HALF]))
        below = dot_nt(low[HALF:], keys[:HALF]).astype(BF16)
        second = causal(dot_nt(low[HALF:], keys[HALF:]))
        inside[:HALF, head(i)] = dot_nn(first, values[:HALF])
        inside[HALF:, head(i)] = dot_nn(below, values[:HALF]) + dot_nn(second, values[HALF:])


def inside_blocks(query, feat_key, value):
    return call(
        inside_body,
        (HEADS // GROUP,),
        [PAIR_SPEC] * 3,
        [PAIR_SPEC] * 2,
        [WIDE_LOW, WIDE],
        1 << 32,
        12 * MIB,
    )(query, feat_key, value)


def scan_body(reverse, pieces, sums):
    peers = pieces.shape[0]
    total = jnp.zeros(pieces.shape[1:], F32)
    for k in reversed(range(peers)) if reverse else range(peers):
        sums[k] = total.astype(BF16)
        total = total + pieces[k].astype(F32)


def exclusive_sums(pieces, reverse):
    peers, rows, lanes = pieces.shape
    part = spec((peers, rows // 2, lanes), lambda i: (0, i, 0))
    return call(
        lambda a, b: scan_body(reverse, a, b),
        (2,),
        [part],
        part,
        jax.ShapeDtypeStruct(pieces.shape, BF16),
        1 << 23,
        MIB,
    )(pieces)


def scanned(block_state, reverse):
    peers = 1
    for axis in SEQ:
        peers *= lax.axis_size(axis)
    pieces = block_state.reshape(peers, -1, HEAD_DIM)
    pieces = lax.all_to_all(pieces, SEQ, 0, 0, tiled=True)
    sums = exclusive_sums(pieces, reverse)
    sums = lax.all_to_all(sums, SEQ, 0, 0, tiled=True)
    return sums.reshape(block_state.shape)


ROW_SPEC = spec((ROWS, FEATURES), lambda i: (i, 0))
EDGE_SPEC = spec((ROWS, HEAD_DIM), lambda i: (i, 0))
GAIN_SPEC = spec((1, FEATURES), lambda i: (0, 0))
ALL_STATES = spec((HEADS, HEAD_DIM, HEAD_DIM), lambda i: (0, 0, 0))
SPLIT_SPEC = spec((2, ROWS, FEATURES // 2), lambda i: (0, i, 0))


def attend_body(inside, feat_query, state, gain, mixed, split, normed, inverse):
    squares = jnp.zeros((ROWS, HEAD_DIM), F32)
    for i in range(HEADS):
        attention = inside[:, head(i)] + dot_nn(feat_query[:, head(i)], state[i])
        normed[:, head(i)] = attention
        squares = squares + attention * attention
    radius = jnp.sqrt(jnp.sum(squares, axis=1, keepdims=True) / FEATURES + epsilon)
    scale = 1.0 / radius
    inverse[...] = jnp.broadcast_to(scale, inverse.shape)
    part = HEAD_DIM // 2
    for i in range(0, HEADS, 2):
        lows = []
        for j in (i, i + 1):
            value = normed[:, head(j)] * scale
            normed[:, head(j)] = value
            low = (value * gain[:, head(j)]).astype(BF16)
            mixed[:, head(j)] = low
            lows.append(low)
        at = head(i // 2)
        split[0, :, at] = jnp.concatenate([lows[0][:, :part], lows[1][:, :part]], axis=1)
        split[1, :, at] = jnp.concatenate([lows[0][:, part:], lows[1][:, part:]], axis=1)


def attend(inside, feat_query, state, gain):
    return call(
        attend_body,
        (BLOCK // ROWS,),
        [ROW_SPEC, ROW_SPEC, ALL_STATES, GAIN_SPEC],
        [ROW_SPEC, SPLIT_SPEC, ROW_SPEC, EDGE_SPEC],
        [
            WIDE_LOW,
            jax.ShapeDtypeStruct((2, BLOCK, FEATURES // 2), BF16),
            WIDE,
            jax.ShapeDtypeStruct((BLOCK, HEAD_DIM), F32),
        ],
        1 << 29,
        15 * MIB,
    )(inside, feat_query, state, gain)


CHUNK = 2 * HEAD_DIM
CHUNKS = FEATURES // CHUNK


CHUNK = 2 * HEAD_DIM
CHUNKS = FEATURES // CHUNK


def norm_back_body(
    place, grad, w0, w1, w2, w3, o0, o1, o2, o3, normed, inverse, gain, feat_query,
    grad_att, state, weight, hats, norms, feats, products
):
    step = pl.program_id(0)

    @pl.when(step == 0)
    def _():
        products[...] = jnp.zeros_like(products)

    part = HEAD_DIM // 2
    for i in range(2):
        rows = slice(i * part, (i + 1) * part)
        for side, pieces in ((place[0], (w0, w1, w2, w3)), (place[1], (o0, o1, o2, o3))):
            at = pl.multiple_of(i * HEAD_DIM + side * part, part)
            for c, piece in enumerate(pieces):
                weight[pl.ds(at, part), c * WIDTH : (c + 1) * WIDTH] = piece[rows]
    hat = dot_nt(grad[...], weight[...]) * gain[...]
    product = hat * normed[...]
    products[...] += product[:, :HEAD_DIM] + product[:, HEAD_DIM:]
    hats[step] = hat
    norms[step] = normed[...]
    feats[step] = feat_query[...]

    @pl.when(step == CHUNKS - 1)
    def _():
        mean = jnp.sum(products[...], axis=1, keepdims=True) / FEATURES
        scale = inverse[:, :1]
        for i in range(HEADS):
            c, at = i // 2, head(i % 2)
            low = ((hats[c, :, at] - norms[c, :, at] * mean) * scale).astype(BF16)
            grad_att[:, head(i)] = low
            state[i] = dot_tn(feats[c, :, at], low).astype(BF16)


def norm_back(place, grad_result, pieces, normed, inverse, gain, feat_query):
    part = spec((BLOCK, CHUNK), lambda i, p: (0, i))
    whole = spec((BLOCK, FEATURES), lambda i, p: (0, 0))
    piece = spec((CHUNK // 2, WIDTH), lambda i, p: (i, 0))
    return pl.pallas_call(
        norm_back_body,
        grid_spec=pltpu.PrefetchScalarGridSpec(
            num_scalar_prefetch=1,
            grid=(CHUNKS,),
            in_specs=[whole]
            + [piece] * 8
            + [
                part,
                spec((BLOCK, HEAD_DIM), lambda i, p: (0, 0)),
                spec((1, CHUNK), lambda i, p: (0, i)),
                part,
            ],
            out_specs=[
                whole,
                spec((HEADS, HEAD_DIM, HEAD_DIM), lambda i, p: (0, 0, 0)),
                spec((CHUNK, FEATURES), lambda i, p: (i, 0)),
            ],
            scratch_shapes=[
                pltpu.VMEM((CHUNKS, BLOCK, CHUNK), F32),
                pltpu.VMEM((CHUNKS, BLOCK, CHUNK), F32),
                pltpu.VMEM((CHUNKS, BLOCK, CHUNK), BF16),
                pltpu.VMEM((BLOCK, HEAD_DIM), F32),
            ],
        ),
        out_shape=[WIDE_LOW, STATE_LOW, jax.ShapeDtypeStruct((FEATURES, FEATURES), BF16)],
        compiler_params=pltpu.CompilerParams(vmem_limit_bytes=60 * MIB),
        cost_estimate=pl.CostEstimate(
            flops=5 << 30, bytes_accessed=26 * MIB, transcendentals=0
        ),
        name="norm_back",
    )(place, grad_result, *(p[0] for p in pieces), *(p[1] for p in pieces), normed, inverse, gain, feat_query)


def back_body(query, feat_query, feat_key, value, grad, state, grad_query, part_key, part_value):
    for i in range(GROUP):
        at = head(i)
        q0, q1 = feat_query[:HALF, at], feat_query[HALF:, at]
        k0, k1 = feat_key[:HALF, at], feat_key[HALF:, at]
        v0, v1 = value[:HALF, at], value[HALF:, at]
        g0, g1 = grad[:HALF, at], grad[HALF:, at]
        s00 = causal(dot_nt(q0, k0))
        s10 = dot_nt(q1, k0).astype(BF16)
        s11 = causal(dot_nt(q1, k1))
        part_value[:HALF, at] = dot_tn(s00, g0) + dot_tn(s10, g1)
        part_value[HALF:, at] = dot_tn(s11, g1)
        d00 = causal(dot_nt(g0, v0))
        d10 = dot_nt(g1, v0).astype(BF16)
        d11 = causal(dot_nt(g1, v1))
        part_key[:HALF, at] = dot_tn(d00, q0) + dot_tn(d10, q1)
        part_key[HALF:, at] = dot_tn(d11, q1)
        fq0 = dot_nn(d00, k0) + dot_nt(g0, state[i])
        fq1 = dot_nn(d10, k0) + dot_nn(d11, k1) + dot_nt(g1, state[i])
        grad_query[:HALF, at] = (fq0 * silu_slope(query[:HALF, at])).astype(BF16)
        grad_query[HALF:, at] = (fq1 * silu_slope(query[HALF:, at])).astype(BF16)


def back_inside(query, feat_query, feat_key, value, grad, state):
    return call(
        back_body,
        (HEADS // GROUP,),
        [PAIR_SPEC] * 5 + [STATE_SPEC],
        [PAIR_SPEC] * 3,
        [WIDE_LOW, WIDE, WIDE],
        3 << 32,
        20 * MIB,
    )(query, feat_query, feat_key, value, grad, state)


def finish_body(key, feat_key, value, part_key, part_value, later, grad_key, grad_value):
    for i in range(GROUP):
        at = head(i)
        fk = part_key[:, at] + dot_nt(value[:, at], later[i])
        grad_key[:, at] = (fk * silu_slope(key[:, at])).astype(BF16)
        grad_value[:, at] = (part_value[:, at] + dot_nn(feat_key[:, at], later[i])).astype(BF16)


def finish(key, feat_key, value, part_key, part_value, later):
    return call(
        finish_body,
        (HEADS // GROUP,),
        [PAIR_SPEC] * 5 + [STATE_SPEC],
        [PAIR_SPEC] * 2,
        [WIDE_LOW, WIDE_LOW],
        1 << 30,
        18 * MIB,
    )(key, feat_key, value, part_key, part_value, later)


def on_ring(low, high):
    return low + high * (3 - 2 * low)


def my_bits(axis):
    at = lax.axis_index(axis)
    high = (at >= 2).astype(jnp.int32)
    low = ((at == 1) | (at == 2)).astype(jnp.int32)
    return (low, high)


def hop(sent, axis, which):
    return lax.ppermute(sent, axis, CYCLES[which])


def product_body(place, left, right, out):
    out[...] = dot_tn(left[0], right[...]).astype(BF16)


def slab_at(color, side, s):
    other, rest, z = s // 16, (s // 4) % 4, s % 4
    z = on_ring(z // 2, z % 2)
    far = on_ring(rest // 2, rest % 2)
    near = on_ring(side, other) if color % 2 == 0 else on_ring(other, side)
    y, x = (far, near) if color < 2 else (near, far)
    return pl.multiple_of((y * 16 + z * 4 + x) * SLAB, SLAB)


def first_body(color, place, left, right, got, kept, sent, acc):
    acc[...] = (dot_tn(left[0], right[...]) + got[...].astype(F32)).astype(BF16)
    bit = place[2 + color]
    for side, out in ((bit, kept), (1 - bit, sent)):
        for s in range(PLACES // 2):
            at = slab_at(color, side, s)
            out[s * SLAB : (s + 1) * SLAB] = acc[pl.ds(at, SLAB)]


def last_body(color, place, mine, got, out):
    bit = place[2 + color]
    for side, part in ((bit, mine), (1 - bit, got)):
        for s in range(PLACES // 2):
            at = slab_at(color, side, s)
            out[pl.ds(at, SLAB)] = part[s * SLAB : (s + 1) * SLAB]


def widened(mine, got, bit):
    low = jnp.where(bit == 0, mine, got)
    high = jnp.where(bit == 0, got, mine)
    return jnp.concatenate([low, high], axis=0)


def own_rows(rows, place, xs, ys, zs):
    for which in (1, 0):
        rows = widened(rows, hop(rows, "seq_1", which), zs[which])
    sides = []
    for near, (bits, axis) in enumerate(((ys, "seq_0"), (xs, "dp"))):
        part = rows[:, near * FEATURES // 2 : (near + 1) * FEATURES // 2]
        for which in (1, 0):
            part = widened(part, hop(part, axis, which), bits[which])
        sides += [part[:, :WIDTH], part[:, WIDTH:]]
    order = ((xs, "dp"), (ys, "seq_0"))
    for color in range(COLORS):
        bits, axis = order[color // 2]
        which = 1 - color % 2
        sides[color] = widened(sides[color], hop(sides[color], axis, which), bits[which])
    half = FEATURES // 2
    part = pl.BlockSpec((half // 2, WIDTH), lambda i, p: (0, 0))
    whole = pl.BlockSpec((half, WIDTH), lambda i, p: (0, 0))
    pieces = []
    for color in range(COLORS):
        axis = order[color // 2][1]
        own = pl.pallas_call(
            lambda *refs, color=color: last_body(color, *refs),
            grid_spec=pltpu.PrefetchScalarGridSpec(
                num_scalar_prefetch=1, grid=(1,), in_specs=[part, part], out_specs=whole
            ),
            out_shape=jax.ShapeDtypeStruct((half, WIDTH), BF16),
            cost_estimate=pl.CostEstimate(flops=1 << 26, bytes_accessed=2 * MIB, transcendentals=0),
            name="last_rows",
        )(place, sides[color], hop(sides[color], axis, color % 2))
        pieces.append((own, lax.ppermute(own, "seq_2", [(0, 1), (1, 0)])))
    return pieces


def gradient_rows(split, grad_result, place, xs, ys, zs):
    half = FEATURES // 2

    def grid_spec(which, color, more, outs):
        return pltpu.PrefetchScalarGridSpec(
            num_scalar_prefetch=1,
            grid=(1,),
            in_specs=[
                pl.BlockSpec((1, BLOCK, half), lambda i, p: (p[which], 0, 0)),
                pl.BlockSpec((BLOCK, WIDTH), lambda i, p: (0, color)),
            ]
            + more,
            out_specs=outs,
            scratch_shapes=[pltpu.VMEM((half, WIDTH), BF16)] if more else [],
        )

    whole = pl.BlockSpec((half, WIDTH), lambda i, p: (0, 0))
    part = pl.BlockSpec((half // 2, WIDTH), lambda i, p: (0, 0))
    params = pltpu.CompilerParams(vmem_limit_bytes=32 * MIB)
    cost = pl.CostEstimate(flops=1 << 30, bytes_accessed=4 * MIB, transcendentals=0)

    gots = []
    for color in range(COLORS):
        sent = pl.pallas_call(
            product_body,
            grid_spec=grid_spec(1, color, [], whole),
            out_shape=jax.ShapeDtypeStruct((half, WIDTH), BF16),
            compiler_params=params,
            cost_estimate=cost,
            name="pair_product",
        )(place, split, grad_result)
        gots.append(lax.ppermute(sent, "seq_2", [(0, 1), (1, 0)]))
    order = ((xs, "dp"), (ys, "seq_0"))
    keeps = []
    for color in range(COLORS):
        kept, sent = pl.pallas_call(
            lambda *refs, color=color: first_body(color, *refs),
            grid_spec=grid_spec(0, color, [whole], [part, part]),
            out_shape=[jax.ShapeDtypeStruct((half // 2, WIDTH), BF16)] * 2,
            compiler_params=params,
            cost_estimate=cost,
            name="first_halves",
        )(place, split, grad_result, gots[color])
        keeps.append((kept, hop(sent, order[color // 2][1], color % 2)))

    def halves(total, bit, axis):
        count = total.shape[axis] // 2
        kept = lax.dynamic_slice_in_dim(total, bit * count, count, axis)
        sent = lax.dynamic_slice_in_dim(total, (1 - bit) * count, count, axis)
        return (kept, sent)

    def add(kept, got):
        return (kept.astype(F32) + got.astype(F32)).astype(BF16)

    seconds = []
    for color, (kept, got) in enumerate(keeps):
        bits, axis = order[color // 2]
        which = 1 - color % 2
        kept, sent = halves(add(kept, got), bits[which], 0)
        seconds.append((kept, hop(sent, axis, which)))
    joined = []
    for near in range(2):
        bits, axis = order[1 - near]
        total = jnp.stack([add(*seconds[2 * near]), add(*seconds[2 * near + 1])])
        for which in range(2):
            kept, sent = halves(total, bits[which], 1)
            total = add(kept, hop(sent, axis, which))
        joined.append(total)
    total = jnp.concatenate(joined, axis=0)
    kept, sent = halves(total, zs[0], 1)
    total = add(kept, hop(sent, "seq_1", 0))
    kept, sent = halves(total, zs[1], 1)
    total = kept.astype(F32) + hop(sent, "seq_1", 1).astype(F32)
    return jnp.concatenate([total[c] for c in range(COLORS)], axis=1)


def layer(query_input, key_input, value_input, grad_output, out_weight, norm_gain):
    query, key, value, grad_result = query_input[0], key_input[0], value_input[0], grad_output[0]
    gain = norm_gain.reshape(1, FEATURES)
    core = lax.axis_index("seq_2")
    xs, ys, zs = my_bits("dp"), my_bits("seq_0"), my_bits("seq_1")
    place = jnp.stack([core, 1 - core, xs[0], xs[1], ys[0], ys[1]]).astype(jnp.int32)
    pieces = own_rows(out_weight, place, xs, ys, zs)
    feat_key, block_kv = block_states(key, value)
    prefix = scanned(block_kv, False)
    feat_query, inside = inside_blocks(query, feat_key, value)
    mixed, split, normed, inverse = attend(inside, feat_query, prefix, gain)
    grad_weight = gradient_rows(split, grad_result, place, xs, ys, zs)
    grad_att, block_grad, full_weight = norm_back(
        place, grad_result, pieces, normed, inverse, gain, feat_query
    )
    later = scanned(block_grad, True)
    result = dot_nn(mixed, full_weight).astype(BF16)
    grad_query, part_key, part_value = back_inside(
        query, feat_query, feat_key, value, grad_att, prefix
    )
    grad_key, grad_value = finish(key, feat_key, value, part_key, part_value, later)
    return (result[None], grad_query[None], grad_key[None], grad_value[None], grad_weight)


def solution(mesh):
    torus = Mesh(mesh.devices.reshape(4, 4, 2, mesh.shape["dp"]), ("seq_0", "seq_1", "seq_2", "dp"))
    placed = (
        P("dp", SEQ, None),
        P("dp", SEQ, None),
        P("dp", SEQ, None),
        P("dp", SEQ, None),
        P(SEQ_DP, None),
        P(),
    )
    return jax.shard_map(
        layer,
        mesh=torus,
        in_specs=placed,
        out_specs=(
            P("dp", SEQ, None),
            P("dp", SEQ, None),
            P("dp", SEQ, None),
            P("dp", SEQ, None),
            P(SEQ_DP, None),
        ),
        check_vma=False,
    )
```

```python
import jax
import jax.numpy as jnp
from jax import lax
from jax.experimental import pallas as pl
from jax.experimental.pallas import tpu as pltpu
from jax.sharding import Mesh
from jax.sharding import PartitionSpec as P


HEADS = 16
HEAD_DIM = 128
BLOCK = 512
HALF = BLOCK // 2
GROUP = 4
PAIR = GROUP * HEAD_DIM
FEATURES = HEADS * HEAD_DIM
ROWS = 128
SEQ = ("seq_0", "seq_1", "seq_2")
SEQ_DP = ("seq_0", "seq_1", "seq_2", "dp")
F32 = jnp.float32
BF16 = jnp.bfloat16


epsilon = 1e-06


def head(i):
    return slice(i * HEAD_DIM, (i + 1) * HEAD_DIM)


def dot_nn(left, right):
    return lax.dot_general(left, right, (((1,), (0,)), ((), ())), preferred_element_type=F32)


def dot_nt(left, right):
    return lax.dot_general(left, right, (((1,), (1,)), ((), ())), preferred_element_type=F32)


def dot_tn(left, right):
    return lax.dot_general(left, right, (((0,), (0,)), ((), ())), preferred_element_type=F32)


def silu_low(raw):
    wide = raw.astype(F32)
    return (wide * jax.nn.sigmoid(wide)).astype(BF16)


def silu_slope(raw):
    wide = raw.astype(F32)
    s = jax.nn.sigmoid(wide)
    return s * (1.0 + wide * (1.0 - s))


def causal(scores):
    row = lax.broadcasted_iota(jnp.int32, scores.shape, 0)
    col = lax.broadcasted_iota(jnp.int32, scores.shape, 1)
    return jnp.where(row >= col, scores, 0.0).astype(BF16)


def spec(shape, index):
    return pl.BlockSpec(shape, index)


def call(body, grid, in_specs, out_specs, out_shape, flops, moved, scratch=()):
    return pl.pallas_call(
        body,
        grid=grid,
        in_specs=in_specs,
        out_specs=out_specs,
        out_shape=out_shape,
        scratch_shapes=scratch,
        compiler_params=pltpu.CompilerParams(vmem_limit_bytes=60 * 1024 * 1024),
        cost_estimate=pl.CostEstimate(flops=flops, bytes_accessed=moved, transcendentals=0),
    )


COLORS = 2
WIDTH = FEATURES // COLORS
SLAB = 16
PLACES = 64
CYCLES = (((0, 1), (1, 0), (2, 3), (3, 2)), ((0, 3), (3, 0), (1, 2), (2, 1)))
PAIR_SPEC = spec((BLOCK, PAIR), lambda i: (0, i))
STATE_SPEC = spec((GROUP, HEAD_DIM, HEAD_DIM), lambda i: (i, 0, 0))
SCORE_SPEC = spec((GROUP, 3, HALF, HALF), lambda i: (i, 0, 0, 0))
WIDE_LOW = jax.ShapeDtypeStruct((BLOCK, FEATURES), BF16)
WIDE = jax.ShapeDtypeStruct((BLOCK, FEATURES), F32)
STATE_LOW = jax.ShapeDtypeStruct((HEADS, HEAD_DIM, HEAD_DIM), BF16)
MIB = 1 << 20


def states_body(key, value, feat_key, state):
    for i in range(GROUP):
        low = silu_low(key[:, head(i)])
        feat_key[:, head(i)] = low
        state[i] = dot_tn(low, value[:, head(i)]).astype(BF16)


def block_states(key, value):
    return call(
        states_body,
        (HEADS // GROUP,),
        [PAIR_SPEC, PAIR_SPEC],
        [PAIR_SPEC, STATE_SPEC],
        [WIDE_LOW, STATE_LOW],
        1 << 29,
        7 * MIB,
    )(key, value)


def inside_body(query, feat_key, value, feat_query, inside, scores):
    for i in range(GROUP):
        low = silu_low(query[:, head(i)])
        feat_query[:, head(i)] = low
        keys = feat_key[:, head(i)]
        values = value[:, head(i)]
        first = causal(dot_nt(low[:HALF], keys[:HALF]))
        below = dot_nt(low[HALF:], keys[:HALF]).astype(BF16)
        second = causal(dot_nt(low[HALF:], keys[HALF:]))
        scores[i, 0], scores[i, 1], scores[i, 2] = first, below, second
        inside[:HALF, head(i)] = dot_nn(first, values[:HALF])
        inside[HALF:, head(i)] = dot_nn(below, values[:HALF]) + dot_nn(second, values[HALF:])


def inside_blocks(query, feat_key, value):
    return call(
        inside_body,
        (HEADS // GROUP,),
        [PAIR_SPEC] * 3,
        [PAIR_SPEC, PAIR_SPEC, SCORE_SPEC],
        [WIDE_LOW, WIDE, jax.ShapeDtypeStruct((HEADS, 3, HALF, HALF), BF16)],
        1 << 32,
        18 * MIB,
    )(query, feat_key, value)


def scan_body(reverse, pieces, sums):
    peers = pieces.shape[0]
    total = jnp.zeros(pieces.shape[1:], F32)
    for k in reversed(range(peers)) if reverse else range(peers):
        sums[k] = total.astype(BF16)
        total = total + pieces[k].astype(F32)


def exclusive_sums(pieces, reverse):
    peers, rows, lanes = pieces.shape
    part = spec((peers, rows // 2, lanes), lambda i: (0, i, 0))
    return call(
        lambda a, b: scan_body(reverse, a, b),
        (2,),
        [part],
        part,
        jax.ShapeDtypeStruct(pieces.shape, BF16),
        1 << 23,
        MIB,
    )(pieces)


def scanned(block_state, reverse):
    peers = 1
    for axis in SEQ:
        peers *= lax.axis_size(axis)
    pieces = block_state.reshape(peers, -1, HEAD_DIM)
    pieces = lax.all_to_all(pieces, SEQ, 0, 0, tiled=True)
    sums = exclusive_sums(pieces, reverse)
    sums = lax.all_to_all(sums, SEQ, 0, 0, tiled=True)
    return sums.reshape(block_state.shape)


ROW_SPEC = spec((ROWS, FEATURES), lambda i: (i, 0))
EDGE_SPEC = spec((ROWS, HEAD_DIM), lambda i: (i, 0))
GAIN_SPEC = spec((1, FEATURES), lambda i: (0, 0))
ALL_STATES = spec((HEADS, HEAD_DIM, HEAD_DIM), lambda i: (0, 0, 0))
SPLIT_SPEC = spec((2, FEATURES // 2, ROWS), lambda i: (0, 0, i))


def attend_body(inside, feat_query, state, gain, mixed, split, normed, inverse):
    squares = jnp.zeros((ROWS, HEAD_DIM), F32)
    for i in range(HEADS):
        attention = inside[:, head(i)] + dot_nn(feat_query[:, head(i)], state[i])
        normed[:, head(i)] = attention
        squares = squares + attention * attention
    radius = jnp.sqrt(jnp.sum(squares, axis=1, keepdims=True) / FEATURES + epsilon)
    scale = 1.0 / radius
    inverse[...] = jnp.broadcast_to(scale, inverse.shape)
    part = HEAD_DIM // 2
    for i in range(0, HEADS, 2):
        lows = []
        for j in (i, i + 1):
            value = normed[:, head(j)] * scale
            normed[:, head(j)] = value
            low = (value * gain[:, head(j)]).astype(BF16)
            mixed[:, head(j)] = low
            lows.append(low)
        at = head(i // 2)
        turned = [low.T for low in lows]
        for side in range(2):
            rows = slice(side * part, (side + 1) * part)
            split[side, at] = jnp.concatenate([turned[0][rows], turned[1][rows]], axis=0)


def attend(inside, feat_query, state, gain):
    return call(
        attend_body,
        (BLOCK // ROWS,),
        [ROW_SPEC, ROW_SPEC, ALL_STATES, GAIN_SPEC],
        [ROW_SPEC, SPLIT_SPEC, ROW_SPEC, EDGE_SPEC],
        [
            WIDE_LOW,
            jax.ShapeDtypeStruct((2, FEATURES // 2, BLOCK), BF16),
            WIDE,
            jax.ShapeDtypeStruct((BLOCK, HEAD_DIM), F32),
        ],
        1 << 29,
        15 * MIB,
    )(inside, feat_query, state, gain)


CHUNK = 2 * HEAD_DIM
CHUNKS = FEATURES // CHUNK


CHUNK = 2 * HEAD_DIM
CHUNKS = FEATURES // CHUNK


def norm_back_body(
    grad, weight, normed, inverse, gain, feat_query, grad_att, state, hats, norms, feats, products
):
    step = pl.program_id(0)

    @pl.when(step == 0)
    def _():
        products[...] = jnp.zeros_like(products)

    hat = dot_nt(grad[...], weight[...]) * gain[...]
    product = hat * normed[...]
    products[...] += product[:, :HEAD_DIM] + product[:, HEAD_DIM:]
    hats[step] = hat
    norms[step] = normed[...]
    feats[step] = feat_query[...]

    @pl.when(step == CHUNKS - 1)
    def _():
        mean = jnp.sum(products[...], axis=1, keepdims=True) / FEATURES
        scale = inverse[:, :1]
        for i in range(HEADS):
            c, at = i // 2, head(i % 2)
            low = ((hats[c, :, at] - norms[c, :, at] * mean) * scale).astype(BF16)
            grad_att[:, head(i)] = low
            state[i] = dot_tn(feats[c, :, at], low).astype(BF16)


def norm_back(grad_result, weight, normed, inverse, gain, feat_query):
    part = spec((BLOCK, CHUNK), lambda i: (0, i))
    whole = spec((BLOCK, FEATURES), lambda i: (0, 0))
    return call(
        norm_back_body,
        (CHUNKS,),
        [
            whole,
            spec((CHUNK, FEATURES), lambda i: (i, 0)),
            part,
            spec((BLOCK, HEAD_DIM), lambda i: (0, 0)),
            spec((1, CHUNK), lambda i: (0, i)),
            part,
        ],
        [whole, ALL_STATES],
        [WIDE_LOW, STATE_LOW],
        5 << 30,
        18 * MIB,
        scratch=[
            pltpu.VMEM((CHUNKS, BLOCK, CHUNK), F32),
            pltpu.VMEM((CHUNKS, BLOCK, CHUNK), F32),
            pltpu.VMEM((CHUNKS, BLOCK, CHUNK), BF16),
            pltpu.VMEM((BLOCK, HEAD_DIM), F32),
        ],
    )(grad_result, weight, normed, inverse, gain, feat_query)


def back_body(
    query, feat_query, feat_key, value, grad, state, scores, grad_query, part_key, part_value
):
    for i in range(GROUP):
        at = head(i)
        q0, q1 = feat_query[:HALF, at], feat_query[HALF:, at]
        k0, k1 = feat_key[:HALF, at], feat_key[HALF:, at]
        v0, v1 = value[:HALF, at], value[HALF:, at]
        g0, g1 = grad[:HALF, at], grad[HALF:, at]
        s00, s10, s11 = scores[i, 0], scores[i, 1], scores[i, 2]
        part_value[:HALF, at] = dot_tn(s00, g0) + dot_tn(s10, g1)
        part_value[HALF:, at] = dot_tn(s11, g1)
        d00 = causal(dot_nt(g0, v0))
        d10 = dot_nt(g1, v0).astype(BF16)
        d11 = causal(dot_nt(g1, v1))
        part_key[:HALF, at] = dot_tn(d00, q0) + dot_tn(d10, q1)
        part_key[HALF:, at] = dot_tn(d11, q1)
        fq0 = dot_nn(d00, k0) + dot_nt(g0, state[i])
        fq1 = dot_nn(d10, k0) + dot_nn(d11, k1) + dot_nt(g1, state[i])
        grad_query[:HALF, at] = (fq0 * silu_slope(query[:HALF, at])).astype(BF16)
        grad_query[HALF:, at] = (fq1 * silu_slope(query[HALF:, at])).astype(BF16)


def back_inside(query, feat_query, feat_key, value, grad, state, scores):
    return call(
        back_body,
        (HEADS // GROUP,),
        [PAIR_SPEC] * 5 + [STATE_SPEC, SCORE_SPEC],
        [PAIR_SPEC] * 3,
        [WIDE_LOW, WIDE, WIDE],
        3 << 32,
        20 * MIB,
    )(query, feat_query, feat_key, value, grad, state, scores)


def finish_body(key, feat_key, value, part_key, part_value, later, grad_key, grad_value):
    for i in range(GROUP):
        at = head(i)
        fk = part_key[:, at] + dot_nt(value[:, at], later[i])
        grad_key[:, at] = (fk * silu_slope(key[:, at])).astype(BF16)
        grad_value[:, at] = (part_value[:, at] + dot_nn(feat_key[:, at], later[i])).astype(BF16)


def finish(key, feat_key, value, part_key, part_value, later):
    return call(
        finish_body,
        (HEADS // GROUP,),
        [PAIR_SPEC] * 5 + [STATE_SPEC],
        [PAIR_SPEC] * 2,
        [WIDE_LOW, WIDE_LOW],
        1 << 30,
        18 * MIB,
    )(key, feat_key, value, part_key, part_value, later)


def on_ring(low, high):
    return low + high * (3 - 2 * low)


def my_bits(axis):
    at = lax.axis_index(axis)
    high = (at >= 2).astype(jnp.int32)
    low = ((at == 1) | (at == 2)).astype(jnp.int32)
    return (low, high)


def hop(sent, axis, which):
    return lax.ppermute(sent, axis, CYCLES[which])


def product_body(place, mine, other, right, *outs):
    for left, parts in ((other, outs[:COLORS]), (mine, outs[COLORS:])):
        for c, out in enumerate(parts):
            out[...] = dot_nn(left[0], right[:, c * WIDTH : (c + 1) * WIDTH]).astype(BF16)


def slab_at(color, side, s):
    other, rest = s // 16, s % 16
    x = on_ring(side, other) if color == 0 else on_ring(other, side)
    return pl.multiple_of((rest * 4 + x) * SLAB, SLAB)


def first_body(color, place, mine, got, kept, sent):
    bit = place[2 + color]
    for side, out in ((bit, kept), (1 - bit, sent)):
        for s in range(PLACES // 2):
            rows = pl.ds(slab_at(color, side, s), SLAB)
            total = mine[rows].astype(F32) + got[rows].astype(F32)
            out[s * SLAB : (s + 1) * SLAB] = total.astype(BF16)


def second_body(color, place, kept, got, rest, sent):
    bit = place[2 + color]
    rows = kept.shape[0] // 2
    for side, out in ((bit, rest), (1 - bit, sent)):
        at = pl.ds(pl.multiple_of(side * rows, rows), rows)
        out[...] = (kept[at].astype(F32) + got[at].astype(F32)).astype(BF16)


def placed_call(body, place, args, in_specs, out_specs, out_shape, flops, moved, grid):
    return pl.pallas_call(
        body,
        grid_spec=pltpu.PrefetchScalarGridSpec(
            num_scalar_prefetch=1, grid=(grid,), in_specs=in_specs, out_specs=out_specs
        ),
        out_shape=out_shape,
        compiler_params=pltpu.CompilerParams(vmem_limit_bytes=60 * MIB),
        cost_estimate=pl.CostEstimate(flops=flops, bytes_accessed=moved, transcendentals=0),
    )(place, *args)


def gradient_rows(split, grad_result):
    core = lax.axis_index("seq_2")
    bits = my_bits("dp")
    place = jnp.stack([core, 1 - core, bits[0], bits[1]]).astype(jnp.int32)
    half = FEATURES // 2
    rows = half // 4

    def block(share):
        return pl.BlockSpec((half // share, WIDTH), lambda i, p: (0, 0))

    def low(share):
        return jax.ShapeDtypeStruct((half // share, WIDTH), BF16)

    products = placed_call(
        product_body,
        place,
        (split, split, grad_result),
        [
            pl.BlockSpec((1, rows, BLOCK), lambda i, p: (p[0], i, 0)),
            pl.BlockSpec((1, rows, BLOCK), lambda i, p: (p[1], i, 0)),
            pl.BlockSpec((BLOCK, FEATURES), lambda i, p: (0, 0)),
        ],
        [pl.BlockSpec((rows, WIDTH), lambda i, p: (i, 0))] * (2 * COLORS),
        [low(1)] * (2 * COLORS),
        1 << 32,
        12 * MIB,
        4,
    )
    gots = [lax.ppermute(p, "seq_2", [(0, 1), (1, 0)]) for p in products[:COLORS]]
    firsts = []
    for color in range(COLORS):
        kept, sent = placed_call(
            lambda *refs, color=color: first_body(color, *refs),
            place,
            (products[COLORS + color], gots[color]),
            [block(1)] * 2,
            [block(2)] * 2,
            [low(2)] * 2,
            1 << 26,
            6 * MIB,
            1,
        )
        firsts.append((kept, hop(sent, "dp", color)))
    seconds = []
    for color, (kept, got) in enumerate(firsts):
        rest, sent = placed_call(
            lambda *refs, color=color: second_body(1 - color, *refs),
            place,
            (kept, got),
            [block(2)] * 2,
            [block(4)] * 2,
            [low(4)] * 2,
            1 << 26,
            3 * MIB,
            1,
        )
        seconds.append((rest, hop(sent, "dp", 1 - color)))
    total = jnp.concatenate(
        [(rest.astype(F32) + got.astype(F32)).astype(BF16) for rest, got in seconds], axis=1
    )
    total = lax.psum_scatter(total, ("seq_0", "seq_1"), scatter_dimension=0, tiled=True)
    return total.astype(F32)


def layer(query_input, key_input, value_input, grad_output, out_weight, norm_gain):
    query, key, value, grad_result = query_input[0], key_input[0], value_input[0], grad_output[0]
    gain = norm_gain.reshape(1, FEATURES)
    full_weight = lax.all_gather(out_weight, SEQ_DP, axis=0, tiled=True)
    feat_key, block_kv = block_states(key, value)
    prefix = scanned(block_kv, False)
    feat_query, inside, scores = inside_blocks(query, feat_key, value)
    mixed, split, normed, inverse = attend(inside, feat_query, prefix, gain)
    grad_weight = gradient_rows(split, grad_result)
    grad_att, block_grad = norm_back(
        grad_result, full_weight, normed, inverse, gain, feat_query
    )
    later = scanned(block_grad, True)
    result = dot_nn(mixed, full_weight).astype(BF16)
    grad_query, part_key, part_value = back_inside(
        query, feat_query, feat_key, value, grad_att, prefix, scores
    )
    grad_key, grad_value = finish(key, feat_key, value, part_key, part_value, later)
    return (result[None], grad_query[None], grad_key[None], grad_value[None], grad_weight)


def solution(mesh):
    torus = Mesh(mesh.devices.reshape(4, 4, 2, mesh.shape["dp"]), ("seq_0", "seq_1", "seq_2", "dp"))
    placed = (
        P("dp", SEQ, None),
        P("dp", SEQ, None),
        P("dp", SEQ, None),
        P("dp", SEQ, None),
        P(SEQ_DP, None),
        P(),
    )
    return jax.shard_map(
        layer,
        mesh=torus,
        in_specs=placed,
        out_specs=(
            P("dp", SEQ, None),
            P("dp", SEQ, None),
            P("dp", SEQ, None),
            P("dp", SEQ, None),
            P(SEQ_DP, None),
        ),
        check_vma=False,
    )
```

```python
import jax
import jax.numpy as jnp
from jax import lax
from jax.experimental import pallas as pl
from jax.experimental.pallas import tpu as pltpu
from jax.sharding import Mesh
from jax.sharding import PartitionSpec as P


HEADS = 16
HEAD_DIM = 128
BLOCK = 512
HALF = BLOCK // 2
GROUP = 4
PAIR = GROUP * HEAD_DIM
FEATURES = HEADS * HEAD_DIM
ROWS = 128
SEQ = ("seq_0", "seq_1", "seq_2")
SEQ_DP = ("seq_0", "seq_1", "seq_2", "dp")
F32 = jnp.float32
BF16 = jnp.bfloat16


epsilon = 1e-06


def head(i):
    return slice(i * HEAD_DIM, (i + 1) * HEAD_DIM)


def dot_nn(left, right):
    return lax.dot_general(left, right, (((1,), (0,)), ((), ())), preferred_element_type=F32)


def dot_nt(left, right):
    return lax.dot_general(left, right, (((1,), (1,)), ((), ())), preferred_element_type=F32)


def dot_tn(left, right):
    return lax.dot_general(left, right, (((0,), (0,)), ((), ())), preferred_element_type=F32)


def silu_low(raw):
    wide = raw.astype(F32)
    return (wide * jax.nn.sigmoid(wide)).astype(BF16)


def silu_slope(raw):
    wide = raw.astype(F32)
    s = jax.nn.sigmoid(wide)
    return s * (1.0 + wide * (1.0 - s))


def causal(scores):
    row = lax.broadcasted_iota(jnp.int32, scores.shape, 0)
    col = lax.broadcasted_iota(jnp.int32, scores.shape, 1)
    return jnp.where(row >= col, scores, 0.0).astype(BF16)


def spec(shape, index):
    return pl.BlockSpec(shape, index)


def call(body, grid, in_specs, out_specs, out_shape, flops, moved, scratch=(), limit=60):
    return pl.pallas_call(
        body,
        grid=grid,
        in_specs=in_specs,
        out_specs=out_specs,
        out_shape=out_shape,
        scratch_shapes=scratch,
        compiler_params=pltpu.CompilerParams(vmem_limit_bytes=limit * 1024 * 1024),
        cost_estimate=pl.CostEstimate(flops=flops, bytes_accessed=moved, transcendentals=0),
    )


COLORS = 2
STRIPES = 4
WIDTH = FEATURES // COLORS
SLAB = 16
PLACES = 64
CYCLES = (((0, 1), (1, 0), (2, 3), (3, 2)), ((0, 3), (3, 0), (1, 2), (2, 1)))
PAIR_SPEC = spec((BLOCK, PAIR), lambda i: (0, i))
STATE_SPEC = spec((GROUP, HEAD_DIM, HEAD_DIM), lambda i: (i, 0, 0))
SCORE_SPEC = spec((GROUP, 3, HALF, HALF), lambda i: (i, 0, 0, 0))
WIDE_LOW = jax.ShapeDtypeStruct((BLOCK, FEATURES), BF16)
WIDE = jax.ShapeDtypeStruct((BLOCK, FEATURES), F32)
STATE_LOW = jax.ShapeDtypeStruct((HEADS, HEAD_DIM, HEAD_DIM), BF16)
MIB = 1 << 20


def states_body(key, value, feat_key, state):
    for i in range(GROUP):
        low = silu_low(key[:, head(i)])
        feat_key[:, head(i)] = low
        state[i] = dot_tn(low, value[:, head(i)]).astype(BF16)


def block_states(key, value):
    return call(
        states_body,
        (HEADS // GROUP,),
        [PAIR_SPEC, PAIR_SPEC],
        [PAIR_SPEC, STATE_SPEC],
        [WIDE_LOW, STATE_LOW],
        1 << 29,
        7 * MIB,
    )(key, value)


def inside_body(query, feat_key, value, feat_query, inside, scores):
    for i in range(GROUP):
        low = silu_low(query[:, head(i)])
        feat_query[:, head(i)] = low
        keys = feat_key[:, head(i)]
        values = value[:, head(i)]
        first = causal(dot_nt(low[:HALF], keys[:HALF]))
        below = dot_nt(low[HALF:], keys[:HALF]).astype(BF16)
        second = causal(dot_nt(low[HALF:], keys[HALF:]))
        scores[i, 0], scores[i, 1], scores[i, 2] = first, below, second
        inside[:HALF, head(i)] = dot_nn(first, values[:HALF])
        inside[HALF:, head(i)] = dot_nn(below, values[:HALF]) + dot_nn(second, values[HALF:])


def inside_blocks(query, feat_key, value):
    return call(
        inside_body,
        (HEADS // GROUP,),
        [PAIR_SPEC] * 3,
        [PAIR_SPEC, PAIR_SPEC, SCORE_SPEC],
        [WIDE_LOW, WIDE, jax.ShapeDtypeStruct((HEADS, 3, HALF, HALF), BF16)],
        1 << 32,
        18 * MIB,
    )(query, feat_key, value)


def scan_body(reverse, pieces, sums):
    peers = pieces.shape[0]
    total = jnp.zeros(pieces.shape[1:], F32)
    for k in reversed(range(peers)) if reverse else range(peers):
        sums[k] = total.astype(BF16)
        total = total + pieces[k].astype(F32)


def exclusive_sums(pieces, reverse):
    peers, rows, lanes = pieces.shape
    part = spec((peers, rows // 2, lanes), lambda i: (0, i, 0))
    return call(
        lambda a, b: scan_body(reverse, a, b),
        (2,),
        [part],
        part,
        jax.ShapeDtypeStruct(pieces.shape, BF16),
        1 << 23,
        MIB,
        limit=8,
    )(pieces)


def scanned(block_state, reverse):
    peers = 1
    for axis in SEQ:
        peers *= lax.axis_size(axis)
    pieces = block_state.reshape(peers, -1, HEAD_DIM)
    pieces = lax.all_to_all(pieces, SEQ, 0, 0, tiled=True)
    sums = exclusive_sums(pieces, reverse)
    sums = lax.all_to_all(sums, SEQ, 0, 0, tiled=True)
    return sums.reshape(block_state.shape)


ROW_SPEC = spec((ROWS, FEATURES), lambda i: (i, 0))
EDGE_SPEC = spec((ROWS, HEAD_DIM), lambda i: (i, 0))
GAIN_SPEC = spec((1, FEATURES), lambda i: (0, 0))
ALL_STATES = spec((HEADS, HEAD_DIM, HEAD_DIM), lambda i: (0, 0, 0))
SPLIT_SPEC = spec((2, FEATURES // 2, ROWS), lambda i: (0, 0, i))


def attend_body(inside, feat_query, state, gain, mixed, split, normed, inverse):
    squares = jnp.zeros((ROWS, HEAD_DIM), F32)
    for i in range(HEADS):
        attention = inside[:, head(i)] + dot_nn(feat_query[:, head(i)], state[i])
        normed[:, head(i)] = attention
        squares = squares + attention * attention
    radius = jnp.sqrt(jnp.sum(squares, axis=1, keepdims=True) / FEATURES + epsilon)
    scale = 1.0 / radius
    inverse[...] = jnp.broadcast_to(scale, inverse.shape)
    part = HEAD_DIM // 2
    for i in range(0, HEADS, 2):
        lows = []
        for j in (i, i + 1):
            value = normed[:, head(j)] * scale
            normed[:, head(j)] = value
            low = (value * gain[:, head(j)]).astype(BF16)
            mixed[:, head(j)] = low
            lows.append(low)
        at = head(i // 2)
        turned = [low.T for low in lows]
        for side in range(2):
            rows = slice(side * part, (side + 1) * part)
            split[side, at] = jnp.concatenate([turned[0][rows], turned[1][rows]], axis=0)


def attend(inside, feat_query, state, gain):
    return call(
        attend_body,
        (BLOCK // ROWS,),
        [ROW_SPEC, ROW_SPEC, ALL_STATES, GAIN_SPEC],
        [ROW_SPEC, SPLIT_SPEC, ROW_SPEC, EDGE_SPEC],
        [
            WIDE_LOW,
            jax.ShapeDtypeStruct((2, FEATURES // 2, BLOCK), BF16),
            WIDE,
            jax.ShapeDtypeStruct((BLOCK, HEAD_DIM), F32),
        ],
        1 << 29,
        15 * MIB,
    )(inside, feat_query, state, gain)


CHUNK = 2 * HEAD_DIM
CHUNKS = FEATURES // CHUNK


CHUNK = 2 * HEAD_DIM
CHUNKS = FEATURES // CHUNK


def norm_back_body(
    grad, weight, normed, inverse, gain, feat_query, grad_att, state, hats, norms, feats, products
):
    step = pl.program_id(0)

    @pl.when(step == 0)
    def _():
        products[...] = jnp.zeros_like(products)

    hat = dot_nt(grad[...], weight[...]) * gain[...]
    product = hat * normed[...]
    products[...] += product[:, :HEAD_DIM] + product[:, HEAD_DIM:]
    hats[step] = hat
    norms[step] = normed[...]
    feats[step] = feat_query[...]

    @pl.when(step == CHUNKS - 1)
    def _():
        mean = jnp.sum(products[...], axis=1, keepdims=True) / FEATURES
        scale = inverse[:, :1]
        for i in range(HEADS):
            c, at = i // 2, head(i % 2)
            low = ((hats[c, :, at] - norms[c, :, at] * mean) * scale).astype(BF16)
            grad_att[:, head(i)] = low
            state[i] = dot_tn(feats[c, :, at], low).astype(BF16)


def norm_back(grad_result, weight, normed, inverse, gain, feat_query):
    part = spec((BLOCK, CHUNK), lambda i: (0, i))
    whole = spec((BLOCK, FEATURES), lambda i: (0, 0))
    return call(
        norm_back_body,
        (CHUNKS,),
        [
            whole,
            spec((CHUNK, FEATURES), lambda i: (i, 0)),
            part,
            spec((BLOCK, HEAD_DIM), lambda i: (0, 0)),
            spec((1, CHUNK), lambda i: (0, i)),
            part,
        ],
        [whole, ALL_STATES],
        [WIDE_LOW, STATE_LOW],
        5 << 30,
        18 * MIB,
        scratch=[
            pltpu.VMEM((CHUNKS, BLOCK, CHUNK), F32),
            pltpu.VMEM((CHUNKS, BLOCK, CHUNK), F32),
            pltpu.VMEM((CHUNKS, BLOCK, CHUNK), BF16),
            pltpu.VMEM((BLOCK, HEAD_DIM), F32),
        ],
    )(grad_result, weight, normed, inverse, gain, feat_query)


def back_body(
    query, feat_query, feat_key, value, grad, state, scores, grad_query, part_key, part_value
):
    for i in range(GROUP):
        at = head(i)
        q0, q1 = feat_query[:HALF, at], feat_query[HALF:, at]
        k0, k1 = feat_key[:HALF, at], feat_key[HALF:, at]
        v0, v1 = value[:HALF, at], value[HALF:, at]
        g0, g1 = grad[:HALF, at], grad[HALF:, at]
        s00, s10, s11 = scores[i, 0], scores[i, 1], scores[i, 2]
        part_value[:HALF, at] = dot_tn(s00, g0) + dot_tn(s10, g1)
        part_value[HALF:, at] = dot_tn(s11, g1)
        d00 = causal(dot_nt(g0, v0))
        d10 = dot_nt(g1, v0).astype(BF16)
        d11 = causal(dot_nt(g1, v1))
        part_key[:HALF, at] = dot_tn(d00, q0) + dot_tn(d10, q1)
        part_key[HALF:, at] = dot_tn(d11, q1)
        fq0 = dot_nn(d00, k0) + dot_nt(g0, state[i])
        fq1 = dot_nn(d10, k0) + dot_nn(d11, k1) + dot_nt(g1, state[i])
        grad_query[:HALF, at] = (fq0 * silu_slope(query[:HALF, at])).astype(BF16)
        grad_query[HALF:, at] = (fq1 * silu_slope(query[HALF:, at])).astype(BF16)


def back_inside(query, feat_query, feat_key, value, grad, state, scores):
    return call(
        back_body,
        (HEADS // GROUP,),
        [PAIR_SPEC] * 5 + [STATE_SPEC, SCORE_SPEC],
        [PAIR_SPEC] * 3,
        [WIDE_LOW, WIDE, WIDE],
        3 << 32,
        20 * MIB,
    )(query, feat_query, feat_key, value, grad, state, scores)


def finish_body(key, feat_key, value, part_key, part_value, later, grad_key, grad_value):
    for i in range(GROUP):
        at = head(i)
        fk = part_key[:, at] + dot_nt(value[:, at], later[i])
        grad_key[:, at] = (fk * silu_slope(key[:, at])).astype(BF16)
        grad_value[:, at] = (part_value[:, at] + dot_nn(feat_key[:, at], later[i])).astype(BF16)


def finish(key, feat_key, value, part_key, part_value, later):
    return call(
        finish_body,
        (HEADS // GROUP,),
        [PAIR_SPEC] * 5 + [STATE_SPEC],
        [PAIR_SPEC] * 2,
        [WIDE_LOW, WIDE_LOW],
        1 << 30,
        18 * MIB,
    )(key, feat_key, value, part_key, part_value, later)


def on_ring(low, high):
    return low + high * (3 - 2 * low)


def my_bits(axis):
    at = lax.axis_index(axis)
    high = (at >= 2).astype(jnp.int32)
    low = ((at == 1) | (at == 2)).astype(jnp.int32)
    return (low, high)


def hop(sent, axis, which):
    return lax.ppermute(sent, axis, CYCLES[which])


def product_body(place, left, right, *outs):
    for c, out in enumerate(outs):
        out[...] = dot_nn(left[0], right[:, c * WIDTH : (c + 1) * WIDTH]).astype(BF16)


def slab_at(color, side, s):
    other, rest = s // 16, s % 16
    y, z = rest // 4, on_ring((rest % 4) // 2, rest % 2)
    x = on_ring(side, other) if color == 0 else on_ring(other, side)
    return pl.multiple_of((y * 16 + z * 4 + x) * SLAB, SLAB)


def first_body(color, place, mine, got, kept, sent):
    bit = place[2 + color]
    for side, out in ((bit, kept), (1 - bit, sent)):
        for s in range(PLACES // 2):
            rows = pl.ds(slab_at(color, side, s), SLAB)
            total = mine[rows].astype(F32) + got[rows].astype(F32)
            out[s * SLAB : (s + 1) * SLAB] = total.astype(BF16)


def second_body(color, place, kept, got, rest, sent):
    bit = place[2 + color]
    rows = kept.shape[0] // 2
    for side, out in ((bit, rest), (1 - bit, sent)):
        at = pl.ds(pl.multiple_of(side * rows, rows), rows)
        out[...] = (kept[at].astype(F32) + got[at].astype(F32)).astype(BF16)


def third_body(place, kept0, got0, kept1, got1, out):
    for c, (kept, got) in enumerate(((kept0, got0), (kept1, got1))):
        total = kept[...].astype(F32) + got[...].astype(F32)
        out[:, c * WIDTH : (c + 1) * WIDTH] = total.astype(BF16)


def placed_call(body, place, args, in_specs, out_specs, out_shape, flops, moved, grid):
    limit = 16 if flops == 1 << 26 else 60
    return pl.pallas_call(
        body,
        grid_spec=pltpu.PrefetchScalarGridSpec(
            num_scalar_prefetch=1, grid=(grid,), in_specs=in_specs, out_specs=out_specs
        ),
        out_shape=out_shape,
        compiler_params=pltpu.CompilerParams(vmem_limit_bytes=limit * MIB),
        cost_estimate=pl.CostEstimate(flops=flops, bytes_accessed=moved, transcendentals=0),
    )(place, *args)


def gradient_rows(split, grad_result):
    core = lax.axis_index("seq_2")
    bits = my_bits("dp")
    place = jnp.stack([core, 1 - core, bits[0], bits[1]]).astype(jnp.int32)
    half = FEATURES // 2
    rows = half // 4

    def block(share):
        return pl.BlockSpec((half // share, WIDTH // STRIPES), lambda i, p: (0, i))

    def low(share):
        return jax.ShapeDtypeStruct((half // share, WIDTH), BF16)

    def products(which):
        return placed_call(
            product_body,
            place,
            (split, grad_result),
            [
                pl.BlockSpec((1, rows, BLOCK), lambda i, p: (p[which], i, 0)),
                pl.BlockSpec((BLOCK, FEATURES), lambda i, p: (0, 0)),
            ],
            [pl.BlockSpec((rows, WIDTH), lambda i, p: (i, 0))] * COLORS,
            [low(1)] * COLORS,
            1 << 31,
            7 * MIB,
            half // rows,
        )

    gots = []
    for sent in products(1):
        gots.append(lax.ppermute(sent, "seq_2", [(0, 1), (1, 0)]))
    mine = products(0)
    firsts = []
    for color in range(COLORS):
        kept, sent = placed_call(
            lambda *refs, color=color: first_body(color, *refs),
            place,
            (mine[color], gots[color]),
            [block(1)] * 2,
            [block(2)] * 2,
            [low(2)] * 2,
            1 << 27,
            6 * MIB,
            STRIPES,
        )
        firsts.append((kept, hop(sent, "dp", color)))
    seconds = []
    for color, (kept, got) in enumerate(firsts):
        rest, sent = placed_call(
            lambda *refs, color=color: second_body(1 - color, *refs),
            place,
            (kept, got),
            [block(2)] * 2,
            [block(4)] * 2,
            [low(4)] * 2,
            1 << 26,
            3 * MIB,
            STRIPES,
        )
        seconds.append((rest, hop(sent, "dp", 1 - color)))
    total = placed_call(
        third_body,
        place,
        seconds[0] + seconds[1],
        [pl.BlockSpec((half // 4, WIDTH), lambda i, p: (0, 0))] * 4,
        pl.BlockSpec((half // 4, FEATURES), lambda i, p: (0, 0)),
        jax.ShapeDtypeStruct((half // 4, FEATURES), BF16),
        1 << 26,
        3 * MIB,
        1,
    )
    total = lax.psum_scatter(total, "seq_0", scatter_dimension=0, tiled=True)
    for which, bit in enumerate(my_bits("seq_1")):
        count = total.shape[0] // 2
        kept = lax.dynamic_slice_in_dim(total, bit * count, count, 0).astype(F32)
        sent = lax.dynamic_slice_in_dim(total, (1 - bit) * count, count, 0)
        total = kept + hop(sent.astype(BF16), "seq_1", which).astype(F32)
    return total


def layer(query_input, key_input, value_input, grad_output, out_weight, norm_gain):
    query, key, value, grad_result = query_input[0], key_input[0], value_input[0], grad_output[0]
    gain = norm_gain.reshape(1, FEATURES)
    full_weight = lax.all_gather(out_weight, SEQ_DP, axis=0, tiled=True)
    feat_key, block_kv = block_states(key, value)
    prefix = scanned(block_kv, False)
    feat_query, inside, scores = inside_blocks(query, feat_key, value)
    mixed, split, normed, inverse = attend(inside, feat_query, prefix, gain)
    grad_weight = gradient_rows(split, grad_result)
    grad_att, block_grad = norm_back(
        grad_result, full_weight, normed, inverse, gain, feat_query
    )
    later = scanned(block_grad, True)
    result = dot_nn(mixed, full_weight).astype(BF16)
    grad_query, part_key, part_value = back_inside(
        query, feat_query, feat_key, value, grad_att, prefix, scores
    )
    grad_key, grad_value = finish(key, feat_key, value, part_key, part_value, later)
    return (result[None], grad_query[None], grad_key[None], grad_value[None], grad_weight)


def solution(mesh):
    torus = Mesh(mesh.devices.reshape(4, 4, 2, mesh.shape["dp"]), ("seq_0", "seq_1", "seq_2", "dp"))
    placed = (
        P("dp", SEQ, None),
        P("dp", SEQ, None),
        P("dp", SEQ, None),
        P("dp", SEQ, None),
        P(SEQ_DP, None),
        P(),
    )
    return jax.shard_map(
        layer,
        mesh=torus,
        in_specs=placed,
        out_specs=(
            P("dp", SEQ, None),
            P("dp", SEQ, None),
            P("dp", SEQ, None),
            P("dp", SEQ, None),
            P(SEQ_DP, None),
        ),
        check_vma=False,
    )
```

```python
import jax
import jax.numpy as jnp
from jax import lax
from jax.experimental import pallas as pl
from jax.experimental.pallas import tpu as pltpu
from jax.sharding import Mesh
from jax.sharding import PartitionSpec as P


HEADS = 16
HEAD_DIM = 128
BLOCK = 512
HALF = BLOCK // 2
GROUP = 4
PAIR = GROUP * HEAD_DIM
FEATURES = HEADS * HEAD_DIM
ROWS = 128
SEQ = ("seq_0", "seq_1", "seq_2")
SEQ_DP = ("seq_0", "seq_1", "seq_2", "dp")
F32 = jnp.float32
BF16 = jnp.bfloat16


epsilon = 1e-06


def head(i):
    return slice(i * HEAD_DIM, (i + 1) * HEAD_DIM)


def dot_nn(left, right):
    return lax.dot_general(left, right, (((1,), (0,)), ((), ())), preferred_element_type=F32)


def dot_nt(left, right):
    return lax.dot_general(left, right, (((1,), (1,)), ((), ())), preferred_element_type=F32)


def dot_tn(left, right):
    return lax.dot_general(left, right, (((0,), (0,)), ((), ())), preferred_element_type=F32)


def silu_low(raw):
    wide = raw.astype(F32)
    return (wide * jax.nn.sigmoid(wide)).astype(BF16)


def silu_slope(raw):
    wide = raw.astype(F32)
    s = jax.nn.sigmoid(wide)
    return s * (1.0 + wide * (1.0 - s))


def causal(scores):
    row = lax.broadcasted_iota(jnp.int32, scores.shape, 0)
    col = lax.broadcasted_iota(jnp.int32, scores.shape, 1)
    return jnp.where(row >= col, scores, 0.0).astype(BF16)


def spec(shape, index):
    return pl.BlockSpec(shape, index)


def call(body, grid, in_specs, out_specs, out_shape, flops, moved, scratch=(), limit=60, aliases=()):
    return pl.pallas_call(
        body,
        grid=grid,
        in_specs=in_specs,
        out_specs=out_specs,
        out_shape=out_shape,
        scratch_shapes=scratch,
        input_output_aliases=dict(aliases),
        compiler_params=pltpu.CompilerParams(vmem_limit_bytes=limit * 1024 * 1024),
        cost_estimate=pl.CostEstimate(flops=flops, bytes_accessed=moved, transcendentals=0),
    )


COLORS = 2
STRIPES = 4
WIDTH = FEATURES // COLORS
SLAB = 16
PLACES = 64
CYCLES = (((0, 1), (1, 0), (2, 3), (3, 2)), ((0, 3), (3, 0), (1, 2), (2, 1)))
PAIR_SPEC = spec((BLOCK, PAIR), lambda i: (0, i))
STATE_SPEC = spec((GROUP, HEAD_DIM, HEAD_DIM), lambda i: (i, 0, 0))
SCORE_SPEC = spec((GROUP, 3, HALF, HALF), lambda i: (i, 0, 0, 0))
WIDE_LOW = jax.ShapeDtypeStruct((BLOCK, FEATURES), BF16)
WIDE = jax.ShapeDtypeStruct((BLOCK, FEATURES), F32)
STATE_LOW = jax.ShapeDtypeStruct((HEADS, HEAD_DIM, HEAD_DIM), BF16)
MIB = 1 << 20


def states_body(key, value, feat_key, state):
    for i in range(GROUP):
        low = silu_low(key[:, head(i)])
        feat_key[:, head(i)] = low
        state[i] = dot_tn(low, value[:, head(i)]).astype(BF16)


def block_states(key, value):
    return call(
        states_body,
        (HEADS // GROUP,),
        [PAIR_SPEC, PAIR_SPEC],
        [PAIR_SPEC, STATE_SPEC],
        [WIDE_LOW, STATE_LOW],
        1 << 29,
        7 * MIB,
    )(key, value)


def inside_body(query, feat_key, value, feat_query, inside, scores):
    for i in range(GROUP):
        low = silu_low(query[:, head(i)])
        feat_query[:, head(i)] = low
        keys = feat_key[:, head(i)]
        values = value[:, head(i)]
        first = causal(dot_nt(low[:HALF], keys[:HALF]))
        below = dot_nt(low[HALF:], keys[:HALF]).astype(BF16)
        second = causal(dot_nt(low[HALF:], keys[HALF:]))
        scores[i, 0], scores[i, 1], scores[i, 2] = first, below, second
        inside[:HALF, head(i)] = dot_nn(first, values[:HALF])
        inside[HALF:, head(i)] = dot_nn(below, values[:HALF]) + dot_nn(second, values[HALF:])


def inside_blocks(query, feat_key, value):
    return call(
        inside_body,
        (HEADS // GROUP,),
        [PAIR_SPEC] * 3,
        [PAIR_SPEC, PAIR_SPEC, SCORE_SPEC],
        [WIDE_LOW, WIDE, jax.ShapeDtypeStruct((HEADS, 3, HALF, HALF), BF16)],
        1 << 32,
        18 * MIB,
    )(query, feat_key, value)


def scan_body(reverse, pieces, sums):
    peers = pieces.shape[0]
    total = jnp.zeros(pieces.shape[1:], F32)
    for k in reversed(range(peers)) if reverse else range(peers):
        sums[k] = total.astype(BF16)
        total = total + pieces[k].astype(F32)


def exclusive_sums(pieces, reverse):
    peers, rows, lanes = pieces.shape
    part = spec((peers, rows // 2, lanes), lambda i: (0, i, 0))
    return call(
        lambda a, b: scan_body(reverse, a, b),
        (2,),
        [part],
        part,
        jax.ShapeDtypeStruct(pieces.shape, BF16),
        1 << 23,
        MIB,
        limit=8,
    )(pieces)


def scanned(block_state, reverse):
    peers = 1
    for axis in SEQ:
        peers *= lax.axis_size(axis)
    pieces = block_state.reshape(peers, -1, HEAD_DIM)
    pieces = lax.all_to_all(pieces, SEQ, 0, 0, tiled=True)
    sums = exclusive_sums(pieces, reverse)
    sums = lax.all_to_all(sums, SEQ, 0, 0, tiled=True)
    return sums.reshape(block_state.shape)


ROW_SPEC = spec((ROWS, FEATURES), lambda i: (i, 0))
EDGE_SPEC = spec((ROWS, HEAD_DIM), lambda i: (i, 0))
GAIN_SPEC = spec((1, FEATURES), lambda i: (0, 0))
ALL_STATES = spec((HEADS, HEAD_DIM, HEAD_DIM), lambda i: (0, 0, 0))
SPLIT_SPEC = spec((2, FEATURES // 2, ROWS), lambda i: (0, 0, i))


def attend_body(inside, feat_query, state, gain, mixed, split, normed, inverse):
    squares = jnp.zeros((ROWS, HEAD_DIM), F32)
    for i in range(HEADS):
        attention = inside[:, head(i)] + dot_nn(feat_query[:, head(i)], state[i])
        normed[:, head(i)] = attention
        squares = squares + attention * attention
    radius = jnp.sqrt(jnp.sum(squares, axis=1, keepdims=True) / FEATURES + epsilon)
    scale = 1.0 / radius
    inverse[...] = jnp.broadcast_to(scale, inverse.shape)
    part = HEAD_DIM // 2
    for i in range(0, HEADS, 2):
        lows = []
        for j in (i, i + 1):
            value = normed[:, head(j)] * scale
            normed[:, head(j)] = value
            low = (value * gain[:, head(j)]).astype(BF16)
            mixed[:, head(j)] = low
            lows.append(low)
        at = head(i // 2)
        turned = [low.T for low in lows]
        for side in range(2):
            rows = slice(side * part, (side + 1) * part)
            split[side, at] = jnp.concatenate([turned[0][rows], turned[1][rows]], axis=0)


def attend(inside, feat_query, state, gain):
    return call(
        attend_body,
        (BLOCK // ROWS,),
        [ROW_SPEC, ROW_SPEC, ALL_STATES, GAIN_SPEC],
        [ROW_SPEC, SPLIT_SPEC, ROW_SPEC, EDGE_SPEC],
        [
            WIDE_LOW,
            jax.ShapeDtypeStruct((2, FEATURES // 2, BLOCK), BF16),
            WIDE,
            jax.ShapeDtypeStruct((BLOCK, HEAD_DIM), F32),
        ],
        1 << 29,
        15 * MIB,
    )(inside, feat_query, state, gain)


CHUNK = 2 * HEAD_DIM
CHUNKS = FEATURES // CHUNK


CHUNK = 2 * HEAD_DIM
CHUNKS = FEATURES // CHUNK


def norm_back_body(
    grad, weight, normed, inverse, gain, feat_query, grad_att, state, hats, norms, feats, products
):
    step = pl.program_id(0)

    @pl.when(step == 0)
    def _():
        products[...] = jnp.zeros_like(products)

    hat = dot_nt(grad[...], weight[...]) * gain[...]
    product = hat * normed[...]
    products[...] += product[:, :HEAD_DIM] + product[:, HEAD_DIM:]
    hats[step] = hat
    norms[step] = normed[...]
    feats[step] = feat_query[...].T

    @pl.when(step == CHUNKS - 1)
    def _():
        mean = jnp.sum(products[...], axis=1, keepdims=True) / FEATURES
        scale = inverse[:, :1]
        for i in range(HEADS):
            c, at = i // 2, head(i % 2)
            low = ((hats[c, :, at] - norms[c, :, at] * mean) * scale).astype(BF16)
            grad_att[:, head(i)] = low
            state[i] = dot_nn(feats[c, at], low).astype(BF16)


def norm_back(grad_result, weight, normed, inverse, gain, feat_query):
    part = spec((BLOCK, CHUNK), lambda i: (0, i))
    whole = spec((BLOCK, FEATURES), lambda i: (0, 0))
    return call(
        norm_back_body,
        (CHUNKS,),
        [
            whole,
            spec((CHUNK, FEATURES), lambda i: (i, 0)),
            part,
            spec((BLOCK, HEAD_DIM), lambda i: (0, 0)),
            spec((1, CHUNK), lambda i: (0, i)),
            part,
        ],
        [whole, ALL_STATES],
        [WIDE_LOW, STATE_LOW],
        5 << 30,
        18 * MIB,
        scratch=[
            pltpu.VMEM((CHUNKS, BLOCK, CHUNK), F32),
            pltpu.VMEM((CHUNKS, BLOCK, CHUNK), F32),
            pltpu.VMEM((CHUNKS, CHUNK, BLOCK), BF16),
            pltpu.VMEM((BLOCK, HEAD_DIM), F32),
        ],
    )(grad_result, weight, normed, inverse, gain, feat_query)


def back_body(
    query, feat_query, feat_key, value, grad, state, scores, grad_query, part_key, part_value
):
    for i in range(GROUP):
        at = head(i)
        q0, q1 = feat_query[:HALF, at], feat_query[HALF:, at]
        k0, k1 = feat_key[:HALF, at], feat_key[HALF:, at]
        v0, v1 = value[:HALF, at], value[HALF:, at]
        g0, g1 = grad[:HALF, at], grad[HALF:, at]
        s00, s10, s11 = scores[i, 0], scores[i, 1], scores[i, 2]
        part_value[:HALF, at] = dot_tn(s00, g0) + dot_tn(s10, g1)
        part_value[HALF:, at] = dot_tn(s11, g1)
        d00 = causal(dot_nt(g0, v0))
        d10 = dot_nt(g1, v0).astype(BF16)
        d11 = causal(dot_nt(g1, v1))
        part_key[:HALF, at] = dot_tn(d00, q0) + dot_tn(d10, q1)
        part_key[HALF:, at] = dot_tn(d11, q1)
        fq0 = dot_nn(d00, k0) + dot_nt(g0, state[i])
        fq1 = dot_nn(d10, k0) + dot_nn(d11, k1) + dot_nt(g1, state[i])
        grad_query[:HALF, at] = (fq0 * silu_slope(query[:HALF, at])).astype(BF16)
        grad_query[HALF:, at] = (fq1 * silu_slope(query[HALF:, at])).astype(BF16)


ANY = pl.BlockSpec(memory_space=pl.ANY)


def parted(body, args, out_shape, flops, moved, first, count, olds):
    pair = spec((BLOCK, PAIR), lambda i: (0, i + first))
    state = spec((GROUP, HEAD_DIM, HEAD_DIM), lambda i: (i + first, 0, 0))
    score = spec((GROUP, 3, HALF, HALF), lambda i: (i + first, 0, 0, 0))
    kinds = {2: pair, 3: state, 4: score}
    given = len(args)

    def run(*refs):
        body(*refs[:given], *refs[given + len(olds) :])

    return call(
        run,
        (count,),
        [kinds[a.ndim] for a in args] + [ANY] * len(olds),
        [pair] * len(out_shape),
        out_shape,
        flops,
        moved,
        aliases=[(given + i, i) for i in range(len(olds))],
    )(*args, *olds)


STEPS = HEADS // GROUP
BACK = 3
FINAL = STEPS - 1


def back_inside(args, first, count, olds=()):
    shapes = [WIDE_LOW, WIDE, WIDE]
    return parted(back_body, args, shapes, 3 << 30, 5 * MIB, first, count, olds)


def finish_body(key, feat_key, value, part_key, part_value, later, grad_key, grad_value):
    for i in range(GROUP):
        at = head(i)
        fk = part_key[:, at] + dot_nt(value[:, at], later[i])
        grad_key[:, at] = (fk * silu_slope(key[:, at])).astype(BF16)
        grad_value[:, at] = (part_value[:, at] + dot_nn(feat_key[:, at], later[i])).astype(BF16)


def finish(args, first, count, olds=()):
    shapes = [WIDE_LOW, WIDE_LOW]
    return parted(finish_body, args, shapes, 1 << 29, 9 * MIB, first, count, olds)


def my_bits(axis):
    at = lax.axis_index(axis)
    high = (at >= 2).astype(jnp.int32)
    low = ((at == 1) | (at == 2)).astype(jnp.int32)
    return (low, high)


def hop(sent, axis, which):
    return lax.ppermute(sent, axis, CYCLES[which])


def product_body(place, left, right, out):
    out[...] = dot_nn(left[0], right[...]).astype(BF16)


def first_body(color, place, mine, got, kept, sent):
    turned = place[2 + color] == 1
    places = PLACES // 4
    for rest in range(places):
        rows = slice(rest * 4 * SLAB, (rest + 1) * 4 * SLAB)
        total = mine[rows].astype(F32) + got[rows].astype(F32)
        x0, x1, x2, x3 = (total[i * SLAB : (i + 1) * SLAB] for i in range(4))
        near = ((x0, x1), (x3, x2)) if color == 0 else ((x0, x3), (x1, x2))
        for other, (low, high) in enumerate(near):
            at = slice((other * places + rest) * SLAB, (other * places + rest + 1) * SLAB)
            kept[at] = jnp.where(turned, high, low).astype(BF16)
            sent[at] = jnp.where(turned, low, high).astype(BF16)


def second_body(color, place, kept, got, rest, sent):
    turned = place[2 + color] == 1
    rows = kept.shape[0] // 2
    low = kept[:rows].astype(F32) + got[:rows].astype(F32)
    high = kept[rows:].astype(F32) + got[rows:].astype(F32)
    rest[...] = jnp.where(turned, high, low).astype(BF16)
    sent[...] = jnp.where(turned, low, high).astype(BF16)


def pick_body(place, rows, *outs):
    for k, out in enumerate(outs):
        at = (place[4] + k) % 4
        out[...] = rows[pl.ds(pl.multiple_of(at * SLAB, SLAB), SLAB)]


def third_body(place, kept0, got0, kept1, got1, out):
    for c, (kept, got) in enumerate(((kept0, got0), (kept1, got1))):
        total = kept[...].astype(F32) + got[...].astype(F32)
        out[:, c * WIDTH : (c + 1) * WIDTH] = total.astype(BF16)


def placed_call(body, place, args, in_specs, out_specs, out_shape, flops, moved, grid):
    limit = 16 if flops == 1 << 26 else 60
    return pl.pallas_call(
        body,
        grid_spec=pltpu.PrefetchScalarGridSpec(
            num_scalar_prefetch=1, grid=(grid,), in_specs=in_specs, out_specs=out_specs
        ),
        out_shape=out_shape,
        compiler_params=pltpu.CompilerParams(vmem_limit_bytes=limit * MIB),
        cost_estimate=pl.CostEstimate(flops=flops, bytes_accessed=moved, transcendentals=0),
    )(place, *args)


def gradient_rows(split, grad_result):
    core = lax.axis_index("seq_2")
    bits = my_bits("dp")
    ring = lax.axis_index("seq_1")
    place = jnp.stack([core, 1 - core, bits[0], bits[1], ring]).astype(jnp.int32)
    half = FEATURES // 2

    def block(share):
        return pl.BlockSpec((half // share, WIDTH // STRIPES), lambda i, p: (0, i))

    def low(share):
        return jax.ShapeDtypeStruct((half // share, WIDTH), BF16)

    def product(which, color):
        columns = WIDTH // 2
        return placed_call(
            product_body,
            place,
            (split, grad_result),
            [
                pl.BlockSpec((1, half, BLOCK), lambda i, p: (p[which], 0, 0)),
                pl.BlockSpec((BLOCK, columns), lambda i, p: (0, 2 * color + i)),
            ],
            pl.BlockSpec((half, columns), lambda i, p: (0, i)),
            low(1),
            1 << 30,
            4 * MIB,
            2,
        )

    gots = []
    for color in range(COLORS):
        gots.append(lax.ppermute(product(1, color), "seq_2", [(0, 1), (1, 0)]))
    mine = [product(0, color) for color in range(COLORS)]
    firsts = []
    for color in range(COLORS):
        kept, sent = placed_call(
            lambda *refs, color=color: first_body(color, *refs),
            place,
            (mine[color], gots[color]),
            [block(1)] * 2,
            [block(2)] * 2,
            [low(2)] * 2,
            1 << 27,
            6 * MIB,
            STRIPES,
        )
        firsts.append((kept, hop(sent, "dp", color)))
    seconds = []
    for color, (kept, got) in enumerate(firsts):
        rest, sent = placed_call(
            lambda *refs, color=color: second_body(1 - color, *refs),
            place,
            (kept, got),
            [block(2)] * 2,
            [block(4)] * 2,
            [low(4)] * 2,
            1 << 26,
            3 * MIB,
            STRIPES,
        )
        seconds.append((rest, hop(sent, "dp", 1 - color)))
    total = placed_call(
        third_body,
        place,
        seconds[0] + seconds[1],
        [pl.BlockSpec((half // 4, WIDTH), lambda i, p: (0, 0))] * 4,
        pl.BlockSpec((half // 4, FEATURES), lambda i, p: (0, 0)),
        jax.ShapeDtypeStruct((half // 4, FEATURES), BF16),
        1 << 26,
        3 * MIB,
        1,
    )
    total = lax.psum_scatter(total, "seq_0", scatter_dimension=0, tiled=True)
    slab = pl.BlockSpec((SLAB, FEATURES), lambda i, p: (0, 0))
    slabs = placed_call(
        pick_body,
        place,
        (total,),
        [pl.BlockSpec((4 * SLAB, FEATURES), lambda i, p: (0, 0))],
        [slab] * 4,
        [jax.ShapeDtypeStruct((SLAB, FEATURES), BF16)] * 4,
        1 << 26,
        MIB,
        1,
    )
    total = slabs[0].astype(F32)
    for k in range(1, 4):
        got = lax.ppermute(slabs[k], "seq_1", [(i, (i + k) % 4) for i in range(4)])
        total = total + got.astype(F32)
    return total


def layer(query_input, key_input, value_input, grad_output, out_weight, norm_gain):
    query, key, value, grad_result = query_input[0], key_input[0], value_input[0], grad_output[0]
    gain = norm_gain.reshape(1, FEATURES)
    full_weight = lax.all_gather(out_weight, SEQ_DP, axis=0, tiled=True)
    feat_key, block_kv = block_states(key, value)
    prefix = scanned(block_kv, False)
    feat_query, inside, scores = inside_blocks(query, feat_key, value)
    mixed, split, normed, inverse = attend(inside, feat_query, prefix, gain)
    grad_weight = gradient_rows(split, grad_result)
    grad_att, block_grad = norm_back(
        grad_result, full_weight, normed, inverse, gain, feat_query
    )
    later = scanned(block_grad, True)
    result = dot_nn(mixed, full_weight).astype(BF16)
    args = (query, feat_query, feat_key, value, grad_att, prefix, scores)
    outs = back_inside(args, 0, BACK)
    grad_query, part_key, part_value = back_inside(args, BACK, STEPS - BACK, outs)
    args = (key, feat_key, value, part_key, part_value, later)
    outs = finish(args, 0, FINAL)
    grad_key, grad_value = finish(args, FINAL, STEPS - FINAL, outs)
    return (result[None], grad_query[None], grad_key[None], grad_value[None], grad_weight)


def solution(mesh):
    torus = Mesh(mesh.devices.reshape(4, 4, 2, mesh.shape["dp"]), ("seq_0", "seq_1", "seq_2", "dp"))
    placed = (
        P("dp", SEQ, None),
        P("dp", SEQ, None),
        P("dp", SEQ, None),
        P("dp", SEQ, None),
        P(SEQ_DP, None),
        P(),
    )
    return jax.shard_map(
        layer,
        mesh=torus,
        in_specs=placed,
        out_specs=(
            P("dp", SEQ, None),
            P("dp", SEQ, None),
            P("dp", SEQ, None),
            P("dp", SEQ, None),
            P(SEQ_DP, None),
        ),
        check_vma=False,
    )
```

```python
import jax
import jax.numpy as jnp
from jax import lax
from jax.experimental import pallas as pl
from jax.experimental.pallas import tpu as pltpu
from jax.sharding import Mesh
from jax.sharding import PartitionSpec as P


HEADS = 16
HEAD_DIM = 128
BLOCK = 512
HALF = BLOCK // 2
GROUP = 4
PAIR = GROUP * HEAD_DIM
FEATURES = HEADS * HEAD_DIM
ROWS = 128
SEQ = ("seq_0", "seq_1", "seq_2")
SEQ_DP = ("seq_0", "seq_1", "seq_2", "dp")
F32 = jnp.float32
BF16 = jnp.bfloat16


epsilon = 1e-06


def head(i):
    return slice(i * HEAD_DIM, (i + 1) * HEAD_DIM)


def dot_nn(left, right):
    return lax.dot_general(left, right, (((1,), (0,)), ((), ())), preferred_element_type=F32)


def dot_nt(left, right):
    return lax.dot_general(left, right, (((1,), (1,)), ((), ())), preferred_element_type=F32)


def dot_tn(left, right):
    return lax.dot_general(left, right, (((0,), (0,)), ((), ())), preferred_element_type=F32)


def silu_low(raw):
    wide = raw.astype(F32)
    return (wide * jax.nn.sigmoid(wide)).astype(BF16)


def silu_slope(raw):
    wide = raw.astype(F32)
    s = jax.nn.sigmoid(wide)
    return s * (1.0 + wide * (1.0 - s))


def causal(scores):
    row = lax.broadcasted_iota(jnp.int32, scores.shape, 0)
    col = lax.broadcasted_iota(jnp.int32, scores.shape, 1)
    return jnp.where(row >= col, scores, 0.0).astype(BF16)


def spec(shape, index):
    return pl.BlockSpec(shape, index)


def call(body, grid, in_specs, out_specs, out_shape, flops, moved, scratch=(), limit=60, aliases=()):
    return pl.pallas_call(
        body,
        grid=grid,
        in_specs=in_specs,
        out_specs=out_specs,
        out_shape=out_shape,
        scratch_shapes=scratch,
        input_output_aliases=dict(aliases),
        compiler_params=pltpu.CompilerParams(vmem_limit_bytes=limit * 1024 * 1024),
        cost_estimate=pl.CostEstimate(flops=flops, bytes_accessed=moved, transcendentals=0),
    )


COLORS = 2
STRIPES = 4
WIDTH = FEATURES // COLORS
SLAB = 16
PLACES = 64
CYCLES = (((0, 1), (1, 0), (2, 3), (3, 2)), ((0, 3), (3, 0), (1, 2), (2, 1)))
PAIR_SPEC = spec((BLOCK, PAIR), lambda i: (0, i))
STATE_SPEC = spec((GROUP, HEAD_DIM, HEAD_DIM), lambda i: (i, 0, 0))
SCORE_SPEC = spec((GROUP, 3, HALF, HALF), lambda i: (i, 0, 0, 0))
WIDE_LOW = jax.ShapeDtypeStruct((BLOCK, FEATURES), BF16)
WIDE = jax.ShapeDtypeStruct((BLOCK, FEATURES), F32)
STATE_LOW = jax.ShapeDtypeStruct((HEADS, HEAD_DIM, HEAD_DIM), BF16)
MIB = 1 << 20


def states_body(key, value, feat_key, state):
    for i in range(GROUP):
        low = silu_low(key[:, head(i)])
        feat_key[:, head(i)] = low
        state[i] = dot_tn(low, value[:, head(i)]).astype(BF16)


def block_states(key, value):
    return call(
        states_body,
        (HEADS // GROUP,),
        [PAIR_SPEC, PAIR_SPEC],
        [PAIR_SPEC, STATE_SPEC],
        [WIDE_LOW, STATE_LOW],
        1 << 29,
        7 * MIB,
    )(key, value)


def inside_body(query, feat_key, value, feat_query, inside, scores):
    for i in range(GROUP):
        low = silu_low(query[:, head(i)])
        feat_query[:, head(i)] = low
        keys = feat_key[:, head(i)]
        values = value[:, head(i)]
        first = causal(dot_nt(low[:HALF], keys[:HALF]))
        below = dot_nt(low[HALF:], keys[:HALF]).astype(BF16)
        second = causal(dot_nt(low[HALF:], keys[HALF:]))
        scores[i, 0], scores[i, 1], scores[i, 2] = first, below, second
        inside[:HALF, head(i)] = dot_nn(first, values[:HALF])
        inside[HALF:, head(i)] = dot_nn(below, values[:HALF]) + dot_nn(second, values[HALF:])


def inside_blocks(query, feat_key, value):
    return call(
        inside_body,
        (HEADS // GROUP,),
        [PAIR_SPEC] * 3,
        [PAIR_SPEC, PAIR_SPEC, SCORE_SPEC],
        [WIDE_LOW, WIDE, jax.ShapeDtypeStruct((HEADS, 3, HALF, HALF), BF16)],
        1 << 32,
        18 * MIB,
    )(query, feat_key, value)


def scan_body(reverse, pieces, sums):
    peers = pieces.shape[0]
    total = jnp.zeros(pieces.shape[1:], F32)
    for k in reversed(range(peers)) if reverse else range(peers):
        sums[k] = total.astype(BF16)
        total = total + pieces[k].astype(F32)


def exclusive_sums(pieces, reverse):
    peers, rows, lanes = pieces.shape
    part = spec((peers, rows // 2, lanes), lambda i: (0, i, 0))
    return call(
        lambda a, b: scan_body(reverse, a, b),
        (2,),
        [part],
        part,
        jax.ShapeDtypeStruct(pieces.shape, BF16),
        1 << 23,
        MIB,
        limit=8,
    )(pieces)


def scanned(block_state, reverse):
    peers = 1
    for axis in SEQ:
        peers *= lax.axis_size(axis)
    pieces = block_state.reshape(peers, -1, HEAD_DIM)
    pieces = lax.all_to_all(pieces, SEQ, 0, 0, tiled=True)
    sums = exclusive_sums(pieces, reverse)
    sums = lax.all_to_all(sums, SEQ, 0, 0, tiled=True)
    return sums.reshape(block_state.shape)


ROW_SPEC = spec((ROWS, FEATURES), lambda i: (i, 0))
EDGE_SPEC = spec((ROWS, HEAD_DIM), lambda i: (i, 0))
GAIN_SPEC = spec((1, FEATURES), lambda i: (0, 0))
ALL_STATES = spec((HEADS, HEAD_DIM, HEAD_DIM), lambda i: (0, 0, 0))
SPLIT_SPEC = spec((2, FEATURES // 2, ROWS), lambda i: (0, 0, i))


def attend_body(inside, feat_query, state, gain, mixed, split, normed, inverse):
    squares = jnp.zeros((ROWS, HEAD_DIM), F32)
    for i in range(HEADS):
        attention = inside[:, head(i)] + dot_nn(feat_query[:, head(i)], state[i])
        normed[:, head(i)] = attention
        squares = squares + attention * attention
    radius = jnp.sqrt(jnp.sum(squares, axis=1, keepdims=True) / FEATURES + epsilon)
    scale = 1.0 / radius
    inverse[...] = jnp.broadcast_to(scale, inverse.shape)
    part = HEAD_DIM // 2
    for i in range(0, HEADS, 2):
        lows = []
        for j in (i, i + 1):
            value = normed[:, head(j)] * scale
            normed[:, head(j)] = value
            low = (value * gain[:, head(j)]).astype(BF16)
            mixed[:, head(j)] = low
            lows.append(low)
        at = head(i // 2)
        turned = [low.T for low in lows]
        for side in range(2):
            rows = slice(side * part, (side + 1) * part)
            split[side, at] = jnp.concatenate([turned[0][rows], turned[1][rows]], axis=0)


def attend(inside, feat_query, state, gain):
    return call(
        attend_body,
        (BLOCK // ROWS,),
        [ROW_SPEC, ROW_SPEC, ALL_STATES, GAIN_SPEC],
        [ROW_SPEC, SPLIT_SPEC, ROW_SPEC, EDGE_SPEC],
        [
            WIDE_LOW,
            jax.ShapeDtypeStruct((2, FEATURES // 2, BLOCK), BF16),
            WIDE,
            jax.ShapeDtypeStruct((BLOCK, HEAD_DIM), F32),
        ],
        1 << 29,
        15 * MIB,
        limit=60,
    )(inside, feat_query, state, gain)


CHUNK = 2 * HEAD_DIM
CHUNKS = FEATURES // CHUNK


CHUNK = 2 * HEAD_DIM
CHUNKS = FEATURES // CHUNK


def norm_back_body(
    grad, weight, normed, inverse, gain, feat_query, grad_att, state, hats, norms, feats, products
):
    step = pl.program_id(0)

    @pl.when(step == 0)
    def _():
        products[...] = jnp.zeros_like(products)

    hat = dot_nt(grad[...], weight[...]) * gain[...]
    product = hat * normed[...]
    products[...] += product[:, :HEAD_DIM] + product[:, HEAD_DIM:]
    hats[step] = hat
    norms[step] = normed[...]
    feats[step] = feat_query[...].T

    @pl.when(step == CHUNKS - 1)
    def _():
        mean = jnp.sum(products[...], axis=1, keepdims=True) / FEATURES
        scale = inverse[:, :1]
        for i in range(HEADS):
            c, at = i // 2, head(i % 2)
            low = ((hats[c, :, at] - norms[c, :, at] * mean) * scale).astype(BF16)
            grad_att[:, head(i)] = low
            state[i] = dot_nn(feats[c, at], low).astype(BF16)


def norm_back(grad_result, weight, normed, inverse, gain, feat_query):
    part = spec((BLOCK, CHUNK), lambda i: (0, i))
    whole = spec((BLOCK, FEATURES), lambda i: (0, 0))
    return call(
        norm_back_body,
        (CHUNKS,),
        [
            whole,
            spec((CHUNK, FEATURES), lambda i: (i, 0)),
            part,
            spec((BLOCK, HEAD_DIM), lambda i: (0, 0)),
            spec((1, CHUNK), lambda i: (0, i)),
            part,
        ],
        [whole, ALL_STATES],
        [WIDE_LOW, STATE_LOW],
        5 << 30,
        18 * MIB,
        scratch=[
            pltpu.VMEM((CHUNKS, BLOCK, CHUNK), F32),
            pltpu.VMEM((CHUNKS, BLOCK, CHUNK), F32),
            pltpu.VMEM((CHUNKS, CHUNK, BLOCK), BF16),
            pltpu.VMEM((BLOCK, HEAD_DIM), F32),
        ],
        limit=60,
    )(grad_result, weight, normed, inverse, gain, feat_query)


def back_body(
    query, feat_query, feat_key, value, grad, state, scores, grad_query, part_key, part_value
):
    for i in range(GROUP):
        at = head(i)
        q0, q1 = feat_query[:HALF, at], feat_query[HALF:, at]
        k0, k1 = feat_key[:HALF, at], feat_key[HALF:, at]
        v0, v1 = value[:HALF, at], value[HALF:, at]
        g0, g1 = grad[:HALF, at], grad[HALF:, at]
        s00, s10, s11 = scores[i, 0], scores[i, 1], scores[i, 2]
        part_value[:HALF, at] = (dot_tn(s00, g0) + dot_tn(s10, g1)).astype(BF16)
        part_value[HALF:, at] = dot_tn(s11, g1).astype(BF16)
        d00 = causal(dot_nt(g0, v0))
        d10 = dot_nt(g1, v0).astype(BF16)
        d11 = causal(dot_nt(g1, v1))
        part_key[:HALF, at] = (dot_tn(d00, q0) + dot_tn(d10, q1)).astype(BF16)
        part_key[HALF:, at] = dot_tn(d11, q1).astype(BF16)
        fq0 = dot_nn(d00, k0) + dot_nt(g0, state[i])
        fq1 = dot_nn(d10, k0) + dot_nn(d11, k1) + dot_nt(g1, state[i])
        grad_query[:HALF, at] = (fq0 * silu_slope(query[:HALF, at])).astype(BF16)
        grad_query[HALF:, at] = (fq1 * silu_slope(query[HALF:, at])).astype(BF16)


ANY = pl.BlockSpec(memory_space=pl.ANY)


def parted(body, args, out_shape, flops, moved, first, count, olds):
    pair = spec((BLOCK, PAIR), lambda i: (0, i + first))
    state = spec((GROUP, HEAD_DIM, HEAD_DIM), lambda i: (i + first, 0, 0))
    score = spec((GROUP, 3, HALF, HALF), lambda i: (i + first, 0, 0, 0))
    kinds = {2: pair, 3: state, 4: score}
    given = len(args)

    def run(*refs):
        body(*refs[:given], *refs[given + len(olds) :])

    return call(
        run,
        (count,),
        [kinds[a.ndim] for a in args] + [ANY] * len(olds),
        [pair] * len(out_shape),
        out_shape,
        flops,
        moved,
        aliases=[(given + i, i) for i in range(len(olds))],
    )(*args, *olds)


STEPS = HEADS // GROUP
BACK = 3
FINAL = STEPS // 2


def back_inside(args, first, count, olds=()):
    shapes = [WIDE_LOW] * 3
    return parted(back_body, args, shapes, 3 << 30, 5 * MIB, first, count, olds)


def finish_body(key, feat_key, value, part_key, part_value, later, grad_key, grad_value):
    for i in range(GROUP):
        at = head(i)
        fk = part_key[:, at].astype(F32) + dot_nt(value[:, at], later[i])
        grad_key[:, at] = (fk * silu_slope(key[:, at])).astype(BF16)
        wide = part_value[:, at].astype(F32) + dot_nn(feat_key[:, at], later[i])
        grad_value[:, at] = wide.astype(BF16)


def finish(args, first, count, olds=()):
    shapes = [WIDE_LOW, WIDE_LOW]
    return parted(finish_body, args, shapes, 1 << 29, 9 * MIB, first, count, olds)


def my_bits(axis):
    at = lax.axis_index(axis)
    high = (at >= 2).astype(jnp.int32)
    low = ((at == 1) | (at == 2)).astype(jnp.int32)
    return (low, high)


def hop(sent, axis, which):
    return lax.ppermute(sent, axis, CYCLES[which])


def product_body(place, left, right, *outs):
    step = pl.program_id(0)
    low = dot_nn(left[0], right[...]).astype(BF16)
    for c, out in enumerate(outs):

        @pl.when(step // 2 == c)
        def _():
            out[...] = low


def first_body(color, place, mine, got, kept, sent):
    turned = place[2 + color] == 1
    places = PLACES // 4
    for rest in range(places):
        rows = slice(rest * 4 * SLAB, (rest + 1) * 4 * SLAB)
        total = mine[rows].astype(F32) + got[rows].astype(F32)
        x0, x1, x2, x3 = (total[i * SLAB : (i + 1) * SLAB] for i in range(4))
        near = ((x0, x1), (x3, x2)) if color == 0 else ((x0, x3), (x1, x2))
        for other, (low, high) in enumerate(near):
            at = slice((other * places + rest) * SLAB, (other * places + rest + 1) * SLAB)
            kept[at] = jnp.where(turned, high, low).astype(BF16)
            sent[at] = jnp.where(turned, low, high).astype(BF16)


def second_body(color, place, kept, got, rest, sent):
    turned = place[2 + color] == 1
    rows = kept.shape[0] // 2
    low = kept[:rows].astype(F32) + got[:rows].astype(F32)
    high = kept[rows:].astype(F32) + got[rows:].astype(F32)
    rest[...] = jnp.where(turned, high, low).astype(BF16)
    sent[...] = jnp.where(turned, low, high).astype(BF16)


def pick_body(place, rows, *outs):
    for k, out in enumerate(outs):
        at = (place[4] + k) % 4
        out[...] = rows[pl.ds(pl.multiple_of(at * SLAB, SLAB), SLAB)]


def third_body(place, kept0, got0, kept1, got1, out):
    for c, (kept, got) in enumerate(((kept0, got0), (kept1, got1))):
        total = kept[...].astype(F32) + got[...].astype(F32)
        out[:, c * WIDTH : (c + 1) * WIDTH] = total.astype(BF16)


def placed_call(body, place, args, in_specs, out_specs, out_shape, flops, moved, grid):
    limit = 16
    return pl.pallas_call(
        body,
        grid_spec=pltpu.PrefetchScalarGridSpec(
            num_scalar_prefetch=1, grid=(grid,), in_specs=in_specs, out_specs=out_specs
        ),
        out_shape=out_shape,
        compiler_params=pltpu.CompilerParams(vmem_limit_bytes=limit * MIB),
        cost_estimate=pl.CostEstimate(flops=flops, bytes_accessed=moved, transcendentals=0),
    )(place, *args)


def gradient_rows(split, grad_result):
    core = lax.axis_index("seq_2")
    bits = my_bits("dp")
    ring = lax.axis_index("seq_1")
    place = jnp.stack([core, 1 - core, bits[0], bits[1], ring]).astype(jnp.int32)
    half = FEATURES // 2

    def block(share):
        return pl.BlockSpec((half // share, WIDTH // STRIPES), lambda i, p: (0, i))

    def low(share):
        return jax.ShapeDtypeStruct((half // share, WIDTH), BF16)

    def products(which):
        columns = WIDTH // 2
        return placed_call(
            product_body,
            place,
            (split, grad_result),
            [
                pl.BlockSpec((1, half, BLOCK), lambda i, p: (p[which], 0, 0)),
                pl.BlockSpec((BLOCK, columns), lambda i, p: (0, i)),
            ],
            [
                pl.BlockSpec((half, columns), lambda i, p: (0, jnp.minimum(i, 1))),
                pl.BlockSpec((half, columns), lambda i, p: (0, jnp.maximum(i - 2, 0))),
            ],
            [low(1)] * COLORS,
            1 << 31,
            7 * MIB,
            4,
        )

    gots = []
    for sent in products(1):
        gots.append(lax.ppermute(sent, "seq_2", [(0, 1), (1, 0)]))
    mine = products(0)
    firsts = []
    for color in range(COLORS):
        kept, sent = placed_call(
            lambda *refs, color=color: first_body(color, *refs),
            place,
            (mine[color], gots[color]),
            [block(1)] * 2,
            [block(2)] * 2,
            [low(2)] * 2,
            1 << 27,
            6 * MIB,
            STRIPES,
        )
        firsts.append((kept, hop(sent, "dp", color)))
    seconds = []
    for color, (kept, got) in enumerate(firsts):
        rest, sent = placed_call(
            lambda *refs, color=color: second_body(1 - color, *refs),
            place,
            (kept, got),
            [block(2)] * 2,
            [block(4)] * 2,
            [low(4)] * 2,
            1 << 26,
            3 * MIB,
            STRIPES,
        )
        seconds.append((rest, hop(sent, "dp", 1 - color)))
    total = placed_call(
        third_body,
        place,
        seconds[0] + seconds[1],
        [pl.BlockSpec((half // 4, WIDTH), lambda i, p: (0, 0))] * 4,
        pl.BlockSpec((half // 4, FEATURES), lambda i, p: (0, 0)),
        jax.ShapeDtypeStruct((half // 4, FEATURES), BF16),
        1 << 26,
        3 * MIB,
        1,
    )
    total = lax.psum_scatter(total, "seq_0", scatter_dimension=0, tiled=True)
    slab = pl.BlockSpec((SLAB, FEATURES), lambda i, p: (0, 0))
    slabs = placed_call(
        pick_body,
        place,
        (total,),
        [pl.BlockSpec((4 * SLAB, FEATURES), lambda i, p: (0, 0))],
        [slab] * 4,
        [jax.ShapeDtypeStruct((SLAB, FEATURES), BF16)] * 4,
        1 << 26,
        MIB,
        1,
    )
    total = slabs[0].astype(F32)
    for k in range(1, 4):
        got = lax.ppermute(slabs[k], "seq_1", [(i, (i + k) % 4) for i in range(4)])
        total = total + got.astype(F32)
    return total


def layer(query_input, key_input, value_input, grad_output, out_weight, norm_gain):
    query, key, value, grad_result = query_input[0], key_input[0], value_input[0], grad_output[0]
    gain = norm_gain.reshape(1, FEATURES)
    full_weight = lax.all_gather(out_weight, SEQ_DP, axis=0, tiled=True)
    feat_key, block_kv = block_states(key, value)
    prefix = scanned(block_kv, False)
    feat_query, inside, scores = inside_blocks(query, feat_key, value)
    mixed, split, normed, inverse = attend(inside, feat_query, prefix, gain)
    grad_weight = gradient_rows(split, grad_result)
    grad_att, block_grad = norm_back(
        grad_result, full_weight, normed, inverse, gain, feat_query
    )
    later = scanned(block_grad, True)
    result = dot_nn(mixed, full_weight).astype(BF16)
    args = (query, feat_query, feat_key, value, grad_att, prefix, scores)
    outs = back_inside(args, 0, BACK)
    grad_query, part_key, part_value = back_inside(args, BACK, STEPS - BACK, outs)
    args = (key, feat_key, value, part_key, part_value, later)
    outs = finish(args, 0, FINAL)
    grad_key, grad_value = finish(args, FINAL, STEPS - FINAL, outs)
    return (result[None], grad_query[None], grad_key[None], grad_value[None], grad_weight)


def solution(mesh):
    torus = Mesh(mesh.devices.reshape(4, 4, 2, mesh.shape["dp"]), ("seq_0", "seq_1", "seq_2", "dp"))
    placed = (
        P("dp", SEQ, None),
        P("dp", SEQ, None),
        P("dp", SEQ, None),
        P("dp", SEQ, None),
        P(SEQ_DP, None),
        P(),
    )
    return jax.shard_map(
        layer,
        mesh=torus,
        in_specs=placed,
        out_specs=(
            P("dp", SEQ, None),
            P("dp", SEQ, None),
            P("dp", SEQ, None),
            P("dp", SEQ, None),
            P(SEQ_DP, None),
        ),
        check_vma=False,
    )
```

```python
import jax
import jax.numpy as jnp
from jax import lax
from jax.experimental import pallas as pl
from jax.experimental.pallas import tpu as pltpu
from jax.sharding import Mesh
from jax.sharding import PartitionSpec as P


HEADS = 16
HEAD_DIM = 128
BLOCK = 512
HALF = BLOCK // 2
GROUP = 4
PAIR = GROUP * HEAD_DIM
FEATURES = HEADS * HEAD_DIM
ROWS = 128
SEQ = ("seq_0", "seq_1", "seq_2")
SEQ_DP = ("seq_0", "seq_1", "seq_2", "dp")
F32 = jnp.float32
BF16 = jnp.bfloat16


epsilon = 1e-06


def head(i):
    return slice(i * HEAD_DIM, (i + 1) * HEAD_DIM)


def dot_nn(left, right):
    return lax.dot_general(left, right, (((1,), (0,)), ((), ())), preferred_element_type=F32)


def dot_nt(left, right):
    return lax.dot_general(left, right, (((1,), (1,)), ((), ())), preferred_element_type=F32)


def dot_tn(left, right):
    return lax.dot_general(left, right, (((0,), (0,)), ((), ())), preferred_element_type=F32)


def silu_low(raw):
    wide = raw.astype(F32)
    return (wide * jax.nn.sigmoid(wide)).astype(BF16)


def silu_slope(raw):
    wide = raw.astype(F32)
    s = jax.nn.sigmoid(wide)
    return s * (1.0 + wide * (1.0 - s))


def causal(scores):
    row = lax.broadcasted_iota(jnp.int32, scores.shape, 0)
    col = lax.broadcasted_iota(jnp.int32, scores.shape, 1)
    return jnp.where(row >= col, scores, 0.0).astype(BF16)


def spec(shape, index):
    return pl.BlockSpec(shape, index)


def call(body, grid, in_specs, out_specs, out_shape, flops, moved, scratch=(), limit=60, aliases=()):
    return pl.pallas_call(
        body,
        grid=grid,
        in_specs=in_specs,
        out_specs=out_specs,
        out_shape=out_shape,
        scratch_shapes=scratch,
        input_output_aliases=dict(aliases),
        compiler_params=pltpu.CompilerParams(vmem_limit_bytes=limit * 1024 * 1024),
        cost_estimate=pl.CostEstimate(flops=flops, bytes_accessed=moved, transcendentals=0),
    )


COLORS = 2
STRIPES = 4
WIDTH = FEATURES // COLORS
SLAB = 16
PLACES = 64
CYCLES = (((0, 1), (1, 0), (2, 3), (3, 2)), ((0, 3), (3, 0), (1, 2), (2, 1)))
PAIR_SPEC = spec((BLOCK, PAIR), lambda i: (0, i))
STATE_SPEC = spec((GROUP, HEAD_DIM, HEAD_DIM), lambda i: (i, 0, 0))
SCORE_SPEC = spec((GROUP, 3, HALF, HALF), lambda i: (i, 0, 0, 0))
WIDE_LOW = jax.ShapeDtypeStruct((BLOCK, FEATURES), BF16)
WIDE = jax.ShapeDtypeStruct((BLOCK, FEATURES), F32)
STATE_LOW = jax.ShapeDtypeStruct((HEADS, HEAD_DIM, HEAD_DIM), BF16)
MIB = 1 << 20


def states_body(key, value, feat_key, state):
    for i in range(GROUP):
        low = silu_low(key[:, head(i)])
        feat_key[:, head(i)] = low
        state[i] = dot_tn(low, value[:, head(i)]).astype(BF16)


def block_states(key, value):
    return call(
        states_body,
        (HEADS // GROUP,),
        [PAIR_SPEC, PAIR_SPEC],
        [PAIR_SPEC, STATE_SPEC],
        [WIDE_LOW, STATE_LOW],
        1 << 29,
        7 * MIB,
    )(key, value)


def inside_body(query, feat_key, value, feat_query, inside, scores):
    for i in range(GROUP):
        low = silu_low(query[:, head(i)])
        feat_query[:, head(i)] = low
        keys = feat_key[:, head(i)]
        values = value[:, head(i)]
        first = causal(dot_nt(low[:HALF], keys[:HALF]))
        below = dot_nt(low[HALF:], keys[:HALF]).astype(BF16)
        second = causal(dot_nt(low[HALF:], keys[HALF:]))
        scores[i, 0], scores[i, 1], scores[i, 2] = first, below, second
        inside[:HALF, head(i)] = dot_nn(first, values[:HALF])
        inside[HALF:, head(i)] = dot_nn(below, values[:HALF]) + dot_nn(second, values[HALF:])


def inside_blocks(query, feat_key, value):
    return call(
        inside_body,
        (HEADS // GROUP,),
        [PAIR_SPEC] * 3,
        [PAIR_SPEC, PAIR_SPEC, SCORE_SPEC],
        [WIDE_LOW, WIDE, jax.ShapeDtypeStruct((HEADS, 3, HALF, HALF), BF16)],
        1 << 32,
        18 * MIB,
    )(query, feat_key, value)


def scan_body(reverse, pieces, sums):
    peers = pieces.shape[0]
    total = jnp.zeros(pieces.shape[1:], F32)
    for k in reversed(range(peers)) if reverse else range(peers):
        sums[k] = total.astype(BF16)
        total = total + pieces[k].astype(F32)


def exclusive_sums(pieces, reverse):
    peers, rows, lanes = pieces.shape
    part = spec((peers, rows // 2, lanes), lambda i: (0, i, 0))
    return call(
        lambda a, b: scan_body(reverse, a, b),
        (2,),
        [part],
        part,
        jax.ShapeDtypeStruct(pieces.shape, BF16),
        1 << 23,
        MIB,
        limit=8,
    )(pieces)


def scanned(block_state, reverse):
    peers = 1
    for axis in SEQ:
        peers *= lax.axis_size(axis)
    pieces = block_state.reshape(peers, -1, HEAD_DIM)
    pieces = lax.all_to_all(pieces, SEQ, 0, 0, tiled=True)
    sums = exclusive_sums(pieces, reverse)
    sums = lax.all_to_all(sums, SEQ, 0, 0, tiled=True)
    return sums.reshape(block_state.shape)


ROW_SPEC = spec((ROWS, FEATURES), lambda i: (i, 0))
EDGE_SPEC = spec((ROWS, HEAD_DIM), lambda i: (i, 0))
GAIN_SPEC = spec((1, FEATURES), lambda i: (0, 0))
ALL_STATES = spec((HEADS, HEAD_DIM, HEAD_DIM), lambda i: (0, 0, 0))
SPLIT_SPEC = spec((2, FEATURES // 2, ROWS), lambda i: (0, 0, i))


def attend_body(inside, feat_query, state, gain, mixed, split, normed, inverse):
    squares = jnp.zeros((ROWS, HEAD_DIM), F32)
    for i in range(HEADS):
        attention = inside[:, head(i)] + dot_nn(feat_query[:, head(i)], state[i])
        normed[:, head(i)] = attention
        squares = squares + attention * attention
    radius = jnp.sqrt(jnp.sum(squares, axis=1, keepdims=True) / FEATURES + epsilon)
    scale = 1.0 / radius
    inverse[...] = jnp.broadcast_to(scale, inverse.shape)
    part = HEAD_DIM // 2
    for i in range(0, HEADS, 2):
        lows = []
        for j in (i, i + 1):
            value = normed[:, head(j)] * scale
            normed[:, head(j)] = value
            low = (value * gain[:, head(j)]).astype(BF16)
            mixed[:, head(j)] = low
            lows.append(low)
        at = head(i // 2)
        turned = [low.T for low in lows]
        for side in range(2):
            rows = slice(side * part, (side + 1) * part)
            split[side, at] = jnp.concatenate([turned[0][rows], turned[1][rows]], axis=0)


def attend(inside, feat_query, state, gain):
    return call(
        attend_body,
        (BLOCK // ROWS,),
        [ROW_SPEC, ROW_SPEC, ALL_STATES, GAIN_SPEC],
        [ROW_SPEC, SPLIT_SPEC, ROW_SPEC, EDGE_SPEC],
        [
            WIDE_LOW,
            jax.ShapeDtypeStruct((2, FEATURES // 2, BLOCK), BF16),
            WIDE,
            jax.ShapeDtypeStruct((BLOCK, HEAD_DIM), F32),
        ],
        1 << 29,
        15 * MIB,
        limit=60,
    )(inside, feat_query, state, gain)


CHUNK = 2 * HEAD_DIM
CHUNKS = FEATURES // CHUNK
AHEAD = 3


CHUNK = 2 * HEAD_DIM
CHUNKS = FEATURES // CHUNK


def norm_back_body(
    grad, weight, normed, inverse, gain, feat_query, grad_att, state,
    weights, hats, norms, feats, products, sems
):
    step = pl.program_id(0)

    def arriving(c):
        rows = pl.ds(pl.multiple_of(c * CHUNK, CHUNK), CHUNK)
        return pltpu.make_async_copy(weight.at[rows], weights.at[c], sems.at[c])

    @pl.when(step == 0)
    def _():
        for c in range(AHEAD):
            arriving(c).start()
        products[...] = jnp.zeros_like(products)

    @pl.when(step + AHEAD < CHUNKS)
    def _():
        arriving(step + AHEAD).start()

    arriving(step).wait()
    hat = dot_nt(grad[...], weights[step]) * gain[...]
    product = hat * normed[...]
    products[...] += product[:, :HEAD_DIM] + product[:, HEAD_DIM:]
    hats[step] = hat
    norms[step] = normed[...]
    feats[step] = feat_query[...].T

    @pl.when(step == CHUNKS - 1)
    def _():
        mean = jnp.sum(products[...], axis=1, keepdims=True) / FEATURES
        scale = inverse[:, :1]
        for i in range(HEADS):
            c, at = i // 2, head(i % 2)
            low = ((hats[c, :, at] - norms[c, :, at] * mean) * scale).astype(BF16)
            grad_att[:, head(i)] = low
            state[i] = dot_nn(feats[c, at], low).astype(BF16)


def norm_back(grad_result, weight, normed, inverse, gain, feat_query):
    part = spec((BLOCK, CHUNK), lambda i: (0, i))
    whole = spec((BLOCK, FEATURES), lambda i: (0, 0))
    return call(
        norm_back_body,
        (CHUNKS,),
        [
            whole,
            pl.BlockSpec(memory_space=pltpu.HBM),
            part,
            spec((BLOCK, HEAD_DIM), lambda i: (0, 0)),
            spec((1, CHUNK), lambda i: (0, i)),
            part,
        ],
        [whole, ALL_STATES],
        [WIDE_LOW, STATE_LOW],
        5 << 30,
        18 * MIB,
        scratch=[
            pltpu.VMEM((CHUNKS, CHUNK, FEATURES), BF16),
            pltpu.VMEM((CHUNKS, BLOCK, CHUNK), F32),
            pltpu.VMEM((CHUNKS, BLOCK, CHUNK), F32),
            pltpu.VMEM((CHUNKS, CHUNK, BLOCK), BF16),
            pltpu.VMEM((BLOCK, HEAD_DIM), F32),
            pltpu.SemaphoreType.DMA((CHUNKS,)),
        ],
        limit=60,
    )(grad_result, weight, normed, inverse, gain, feat_query)


def back_body(
    query, feat_query, feat_key, value, grad, state, scores, grad_query, part_key, part_value
):
    for i in range(GROUP):
        at = head(i)
        q0, q1 = feat_query[:HALF, at], feat_query[HALF:, at]
        k0, k1 = feat_key[:HALF, at], feat_key[HALF:, at]
        v0, v1 = value[:HALF, at], value[HALF:, at]
        g0, g1 = grad[:HALF, at], grad[HALF:, at]
        s00, s10, s11 = scores[i, 0], scores[i, 1], scores[i, 2]
        part_value[:HALF, at] = (dot_tn(s00, g0) + dot_tn(s10, g1)).astype(BF16)
        part_value[HALF:, at] = dot_tn(s11, g1).astype(BF16)
        d00 = causal(dot_nt(g0, v0))
        d10 = dot_nt(g1, v0).astype(BF16)
        d11 = causal(dot_nt(g1, v1))
        part_key[:HALF, at] = (dot_tn(d00, q0) + dot_tn(d10, q1)).astype(BF16)
        part_key[HALF:, at] = dot_tn(d11, q1).astype(BF16)
        fq0 = dot_nn(d00, k0) + dot_nt(g0, state[i])
        fq1 = dot_nn(d10, k0) + dot_nn(d11, k1) + dot_nt(g1, state[i])
        grad_query[:HALF, at] = (fq0 * silu_slope(query[:HALF, at])).astype(BF16)
        grad_query[HALF:, at] = (fq1 * silu_slope(query[HALF:, at])).astype(BF16)


ANY = pl.BlockSpec(memory_space=pl.ANY)


def parted(body, args, out_shape, flops, moved, first, count, olds):
    pair = spec((BLOCK, PAIR), lambda i: (0, i + first))
    state = spec((GROUP, HEAD_DIM, HEAD_DIM), lambda i: (i + first, 0, 0))
    score = spec((GROUP, 3, HALF, HALF), lambda i: (i + first, 0, 0, 0))
    kinds = {2: pair, 3: state, 4: score}
    given = len(args)

    def run(*refs):
        body(*refs[:given], *refs[given + len(olds) :])

    return call(
        run,
        (count,),
        [kinds[a.ndim] for a in args] + [ANY] * len(olds),
        [pair] * len(out_shape),
        out_shape,
        flops,
        moved,
        aliases=[(given + i, i) for i in range(len(olds))],
    )(*args, *olds)


STEPS = HEADS // GROUP
BACK = 3
FINAL = STEPS // 2


def back_inside(args, first, count, olds=()):
    shapes = [WIDE_LOW] * 3
    return parted(back_body, args, shapes, 3 << 30, 5 * MIB, first, count, olds)


def finish_body(key, feat_key, value, part_key, part_value, later, grad_key, grad_value):
    for i in range(GROUP):
        at = head(i)
        fk = part_key[:, at].astype(F32) + dot_nt(value[:, at], later[i])
        grad_key[:, at] = (fk * silu_slope(key[:, at])).astype(BF16)
        wide = part_value[:, at].astype(F32) + dot_nn(feat_key[:, at], later[i])
        grad_value[:, at] = wide.astype(BF16)


def finish(args, first, count, olds=()):
    shapes = [WIDE_LOW, WIDE_LOW]
    return parted(finish_body, args, shapes, 1 << 29, 9 * MIB, first, count, olds)


def my_bits(axis):
    at = lax.axis_index(axis)
    high = (at >= 2).astype(jnp.int32)
    low = ((at == 1) | (at == 2)).astype(jnp.int32)
    return (low, high)


def hop(sent, axis, which):
    return lax.ppermute(sent, axis, CYCLES[which])


def product_body(place, left, right, *outs):
    step = pl.program_id(0)
    low = dot_nn(left[0], right[...]).astype(BF16)
    for c, out in enumerate(outs):

        @pl.when(step // 2 == c)
        def _():
            out[...] = low


def first_body(color, place, mine, got, kept, sent):
    turned = place[2 + color] == 1
    places = PLACES // 4
    for rest in range(places):
        rows = slice(rest * 4 * SLAB, (rest + 1) * 4 * SLAB)
        total = mine[rows].astype(F32) + got[rows].astype(F32)
        x0, x1, x2, x3 = (total[i * SLAB : (i + 1) * SLAB] for i in range(4))
        near = ((x0, x1), (x3, x2)) if color == 0 else ((x0, x3), (x1, x2))
        for other, (low, high) in enumerate(near):
            at = slice((other * places + rest) * SLAB, (other * places + rest + 1) * SLAB)
            kept[at] = jnp.where(turned, high, low).astype(BF16)
            sent[at] = jnp.where(turned, low, high).astype(BF16)


def second_body(color, place, kept, got, rest, sent):
    turned = place[2 + color] == 1
    rows = kept.shape[0] // 2
    low = kept[:rows].astype(F32) + got[:rows].astype(F32)
    high = kept[rows:].astype(F32) + got[rows:].astype(F32)
    rest[...] = jnp.where(turned, high, low).astype(BF16)
    sent[...] = jnp.where(turned, low, high).astype(BF16)


def pick_body(place, rows, *outs):
    for k, out in enumerate(outs):
        at = (place[4] + k) % 4
        out[...] = rows[pl.ds(pl.multiple_of(at * SLAB, SLAB), SLAB)]


def third_body(place, kept0, got0, kept1, got1, out):
    for c, (kept, got) in enumerate(((kept0, got0), (kept1, got1))):
        total = kept[...].astype(F32) + got[...].astype(F32)
        out[:, c * WIDTH : (c + 1) * WIDTH] = total.astype(BF16)


def placed_call(body, place, args, in_specs, out_specs, out_shape, flops, moved, grid):
    limit = 16
    return pl.pallas_call(
        body,
        grid_spec=pltpu.PrefetchScalarGridSpec(
            num_scalar_prefetch=1, grid=(grid,), in_specs=in_specs, out_specs=out_specs
        ),
        out_shape=out_shape,
        compiler_params=pltpu.CompilerParams(vmem_limit_bytes=limit * MIB),
        cost_estimate=pl.CostEstimate(flops=flops, bytes_accessed=moved, transcendentals=0),
    )(place, *args)


def gradient_rows(split, grad_result):
    core = lax.axis_index("seq_2")
    bits = my_bits("dp")
    ring = lax.axis_index("seq_1")
    place = jnp.stack([core, 1 - core, bits[0], bits[1], ring]).astype(jnp.int32)
    half = FEATURES // 2

    def block(share):
        return pl.BlockSpec((half // share, WIDTH // STRIPES), lambda i, p: (0, i))

    def low(share):
        return jax.ShapeDtypeStruct((half // share, WIDTH), BF16)

    def products(which):
        columns = WIDTH // 2
        return placed_call(
            product_body,
            place,
            (split, grad_result),
            [
                pl.BlockSpec((1, half, BLOCK), lambda i, p: (p[which], 0, 0)),
                pl.BlockSpec((BLOCK, columns), lambda i, p: (0, i)),
            ],
            [
                pl.BlockSpec((half, columns), lambda i, p: (0, jnp.minimum(i, 1))),
                pl.BlockSpec((half, columns), lambda i, p: (0, jnp.maximum(i - 2, 0))),
            ],
            [low(1)] * COLORS,
            1 << 31,
            7 * MIB,
            4,
        )

    gots = []
    for sent in products(1):
        gots.append(lax.ppermute(sent, "seq_2", [(0, 1), (1, 0)]))
    mine = products(0)
    firsts = []
    for color in range(COLORS):
        kept, sent = placed_call(
            lambda *refs, color=color: first_body(color, *refs),
            place,
            (mine[color], gots[color]),
            [block(1)] * 2,
            [block(2)] * 2,
            [low(2)] * 2,
            1 << 27,
            6 * MIB,
            STRIPES,
        )
        firsts.append((kept, hop(sent, "dp", color)))
    seconds = []
    for color, (kept, got) in enumerate(firsts):
        rest, sent = placed_call(
            lambda *refs, color=color: second_body(1 - color, *refs),
            place,
            (kept, got),
            [block(2)] * 2,
            [block(4)] * 2,
            [low(4)] * 2,
            1 << 26,
            3 * MIB,
            STRIPES,
        )
        seconds.append((rest, hop(sent, "dp", 1 - color)))
    total = placed_call(
        third_body,
        place,
        seconds[0] + seconds[1],
        [pl.BlockSpec((half // 4, WIDTH), lambda i, p: (0, 0))] * 4,
        pl.BlockSpec((half // 4, FEATURES), lambda i, p: (0, 0)),
        jax.ShapeDtypeStruct((half // 4, FEATURES), BF16),
        1 << 26,
        3 * MIB,
        1,
    )
    total = lax.psum_scatter(total, "seq_0", scatter_dimension=0, tiled=True)
    slab = pl.BlockSpec((SLAB, FEATURES), lambda i, p: (0, 0))
    slabs = placed_call(
        pick_body,
        place,
        (total,),
        [pl.BlockSpec((4 * SLAB, FEATURES), lambda i, p: (0, 0))],
        [slab] * 4,
        [jax.ShapeDtypeStruct((SLAB, FEATURES), BF16)] * 4,
        1 << 26,
        MIB,
        1,
    )
    total = slabs[0].astype(F32)
    for k in range(1, 4):
        got = lax.ppermute(slabs[k], "seq_1", [(i, (i + k) % 4) for i in range(4)])
        total = total + got.astype(F32)
    return total


def layer(query_input, key_input, value_input, grad_output, out_weight, norm_gain):
    query, key, value, grad_result = query_input[0], key_input[0], value_input[0], grad_output[0]
    gain = norm_gain.reshape(1, FEATURES)
    full_weight = lax.all_gather(out_weight, SEQ_DP, axis=0, tiled=True)
    feat_key, block_kv = block_states(key, value)
    prefix = scanned(block_kv, False)
    feat_query, inside, scores = inside_blocks(query, feat_key, value)
    mixed, split, normed, inverse = attend(inside, feat_query, prefix, gain)
    grad_weight = gradient_rows(split, grad_result)
    grad_att, block_grad = norm_back(
        grad_result, full_weight, normed, inverse, gain, feat_query
    )
    later = scanned(block_grad, True)
    result = dot_nn(mixed, full_weight).astype(BF16)
    args = (query, feat_query, feat_key, value, grad_att, prefix, scores)
    outs = back_inside(args, 0, BACK)
    grad_query, part_key, part_value = back_inside(args, BACK, STEPS - BACK, outs)
    args = (key, feat_key, value, part_key, part_value, later)
    outs = finish(args, 0, FINAL)
    grad_key, grad_value = finish(args, FINAL, STEPS - FINAL, outs)
    return (result[None], grad_query[None], grad_key[None], grad_value[None], grad_weight)


def solution(mesh):
    torus = Mesh(mesh.devices.reshape(4, 4, 2, mesh.shape["dp"]), ("seq_0", "seq_1", "seq_2", "dp"))
    placed = (
        P("dp", SEQ, None),
        P("dp", SEQ, None),
        P("dp", SEQ, None),
        P("dp", SEQ, None),
        P(SEQ_DP, None),
        P(),
    )
    return jax.shard_map(
        layer,
        mesh=torus,
        in_specs=placed,
        out_specs=(
            P("dp", SEQ, None),
            P("dp", SEQ, None),
            P("dp", SEQ, None),
            P("dp", SEQ, None),
            P(SEQ_DP, None),
        ),
        check_vma=False,
    )
```
